128 devices in a mesh: parts: 1, data: 128 (over z, y, x, core).
Axes of the slice: x: 4, y: 4, z: 4, core: 2. Of those that a mesh axis runs over, the one named last changes fastest.
Arguments:
- feats: bfloat16 [131072, 123], P('data')
- labels: int32 [131072], P('data')
- w_in: float32 [123, 64, 50], P(None, 'parts')
- w_out: float32 [64, 50], P('parts')
- mom_in: float32 [123, 64, 50], P(None, 'parts')
- mom_out: float32 [64, 50], P('parts')
Outputs:
- output 1: float32 [123, 64, 50], P(None, 'parts')
- output 2: float32 [64, 50], P('parts')
- output 3: float32 [123, 64, 50], P(None, 'parts')
- output 4: float32 [64, 50], P('parts')
- output 5: float32 [64], P('parts')
All inputs are finite; a program needn't handle non-finite values.
Results may differ from the reference program's by a relative error of at most 0.001.
Values are sent between devices in bfloat16 or wider.
A program may use at most 1 GiB of HBM per device.

```python
import math
import jax
import jax.numpy as jnp
from jax import lax

D = 123
HIDDEN = 50
CHAINS = 64
ROWS_DEV = 1024
GROUP = 128
LEAPS = 16
N_ROWS = ROWS_DEV * GROUP
STEP = 1.0 / math.sqrt(N_ROWS * (D + HIDDEN))
PRIOR_VAR = 1.0


def setup_inputs(seed: int = 0, part: int = 0) -> dict:
    key = jax.random.key(seed)
    key_mean, key_noise, key_rate, key_draw, key_part = jax.random.split(key, 5)
    centers = jax.random.normal(key_mean, (GROUP, 1, D), jnp.float32)
    noise = jax.random.normal(key_noise, (GROUP, ROWS_DEV, D), jnp.float32)
    feats = (centers + noise).reshape(N_ROWS, D).astype(jnp.bfloat16)
    rates = jax.random.randint(key_rate, (GROUP, 1), 50, 951)
    draws = jax.random.randint(key_draw, (GROUP, ROWS_DEV), 0, 1000)
    labels = (draws < rates).astype(jnp.int32).reshape(N_ROWS)
    part_key = jax.random.fold_in(key_part, part)
    key_w1, key_w2, key_m1, key_m2 = jax.random.split(part_key, 4)
    w_in = jax.random.normal(key_w1, (D, CHAINS, HIDDEN), jnp.float32) * (2.0 * D) ** -0.5
    w_out = jax.random.normal(key_w2, (CHAINS, HIDDEN), jnp.float32) * (1.5 * HIDDEN ** -0.5)
    mom_in = jax.random.normal(key_m1, (D, CHAINS, HIDDEN), jnp.float32)
    mom_out = jax.random.normal(key_m2, (CHAINS, HIDDEN), jnp.float32)
    return {'feats': feats, 'labels': labels, 'w_in': w_in, 'w_out': w_out, 'mom_in': mom_in, 'mom_out': mom_out}


def block_terms(x_rows, lab_rows, w_flat, w_out):
    pre_act = jnp.dot(x_rows, w_flat, preferred_element_type=jnp.float32).reshape(ROWS_DEV, CHAINS, HIDDEN)
    hidden_act = jnp.tanh(pre_act)
    logits = jnp.sum(hidden_act * w_out, axis=-1)
    residual = lab_rows[:, None] - jax.nn.sigmoid(logits)
    grad_out = jnp.sum(hidden_act * residual[:, :, None], axis=0)
    back_grad = (residual[:, :, None] * w_out * (1.0 - hidden_act * hidden_act)).astype(jnp.bfloat16)
    grad_in = jnp.dot(x_rows.T, back_grad.reshape(ROWS_DEV, CHAINS * HIDDEN), preferred_element_type=jnp.float32)
    return grad_in.reshape(D, CHAINS, HIDDEN), grad_out, logits


def log_post_grad(x_blocks, lab_blocks, w_in, w_out):
    w_flat = w_in.astype(jnp.bfloat16).reshape(D, CHAINS * HIDDEN)

    def row_block(acc_sum, block_in):
        grad_in, grad_out, logits = block_terms(block_in[0], block_in[1], w_flat, w_out)
        return (acc_sum[0] + grad_in, acc_sum[1] + grad_out), logits

    sums, logits = lax.scan(row_block, (jnp.zeros_like(w_in), jnp.zeros_like(w_out)), (x_blocks, lab_blocks))
    return sums[0] - w_in / PRIOR_VAR, sums[1] - w_out / PRIOR_VAR, logits


def reference(feats, labels, w_in, w_out, mom_in, mom_out):
    x_blocks = feats.reshape(GROUP, ROWS_DEV, D)
    lab_blocks = labels.astype(jnp.float32).reshape(GROUP, ROWS_DEV)
    grad_in, grad_out, logits = log_post_grad(x_blocks, lab_blocks, w_in, w_out)
    mom_in = mom_in + 0.5 * STEP * grad_in
    mom_out = mom_out + 0.5 * STEP * grad_out

    def leap_step(state_now, unused):
        pos_in, pos_out, vel_in, vel_out = state_now
        pos_in = pos_in + STEP * vel_in
        pos_out = pos_out + STEP * vel_out
        g_in, g_out, g_logits = log_post_grad(x_blocks, lab_blocks, pos_in, pos_out)
        return (pos_in, pos_out, vel_in + STEP * g_in, vel_out + STEP * g_out), None

    state_end, unused_out = lax.scan(leap_step, (w_in, w_out, mom_in, mom_out), None, length=LEAPS - 1)
    pos_in, pos_out, vel_in, vel_out = state_end
    pos_in = pos_in + STEP * vel_in
    pos_out = pos_out + STEP * vel_out
    grad_in, grad_out, logits = log_post_grad(x_blocks, lab_blocks, pos_in, pos_out)
    vel_in = vel_in + 0.5 * STEP * grad_in
    vel_out = vel_out + 0.5 * STEP * grad_out
    row_loss = jnp.sum(jax.nn.softplus(logits) - lab_blocks[:, :, None] * logits, axis=(0, 1))
    energy = row_loss + (jnp.sum(pos_in * pos_in, axis=(0, 2)) + jnp.sum(pos_out * pos_out, axis=1)) / (2.0 * PRIOR_VAR) + 0.5 * (jnp.sum(vel_in * vel_in, axis=(0, 2)) + jnp.sum(vel_out * vel_out, axis=1))
    return pos_in, pos_out, vel_in, vel_out, energy
```

```python
import functools
import math

import jax
import jax.numpy as jnp
from jax import lax
from jax.experimental import pallas as pl
from jax.experimental.pallas import tpu as pltpu
from jax.sharding import PartitionSpec as P

LEAPS = 16
PRIOR_VAR = 1.0
SIDE = 4
BLOCKS = SIDE ** 3
HID = 56
LANES = 128
LAB = 123
LOSS = 124
OUT = 127
ROW_PIECES = ((0, 352, 176), (352, 336, 176), (688, 336, 176))
OUT_PIECES = ((0, 24, 16), (24, 16, 8), (40, 16, 8))


def torus_gather(buf, pieces, coords, device_at, send_sem, recv_sem, barrier=None):
    descs = []
    plus = lambda c, d: lax.rem(c + d + SIDE, SIDE)

    def view(p, where, part):
        start, size, first = pieces[p]
        lo, n = {0: (start, size), 1: (start, first), 2: (start + first, size - first)}[part]
        return buf.at[where[0], where[1], where[2], pl.ds(lo, n), :]

    def copy(p, where, part, axis, step, slot):
        to = list(coords)
        to[axis] = plus(to[axis], step)
        ref = view(p, where, part)
        return pltpu.make_async_remote_copy(
            src_ref=ref, dst_ref=ref, send_sem=send_sem.at[p, slot], recv_sem=recv_sem.at[p, slot],
            device_id={'data': device_at(to)}, device_id_type=pl.DeviceIdType.MESH)

    def send(p, where, part, axis, step, slot):
        c = copy(p, where, part, axis, step, slot)
        c.start()
        descs.append(c)

    def wait(p, where, part, axis, step, slot):
        copy(p, where, part, axis, step, slot).wait_recv()

    orders = [(p, (p + 1) % 3, (p + 2) % 3) for p in range(3)]
    OFFS = (0, -1, 1, 2)

    def at(p, off0, off1, off2):
        where = [None, None, None]
        for axis, off in zip(orders[p], (off0, off1, off2)):
            where[axis] = slice(None) if off is None else (coords[axis] if off == 0 else plus(coords[axis], off))
        return where

    def start_full(p, ph, own, base):
        axis = orders[p][ph]
        send(p, own, 0, axis, 1, base)
        send(p, own, 0, axis, -1, base + 1)

    def relay(p, ph, low, high, base):
        axis = orders[p][ph]
        wait(p, low, 0, axis, 1, base)
        send(p, low, 1, axis, 1, base + 2)
        wait(p, high, 0, axis, 1, base + 1)
        send(p, high, 2, axis, -1, base + 3)

    def finish(p, ph, far, base):
        axis = orders[p][ph]
        wait(p, far, 1, axis, 1, base + 2)
        wait(p, far, 2, axis, 1, base + 3)

    B1, B2, B3 = 0, 4, 20
    for p in range(3):
        start_full(p, 0, at(p, 0, 0, 0), B1)
    for p in range(3):
        start_full(p, 1, at(p, 0, 0, 0), B2)
    for p in range(3):
        relay(p, 0, at(p, -1, 0, 0), at(p, 1, 0, 0), B1)
        start_full(p, 1, at(p, -1, 0, 0), B2 + 4)
        start_full(p, 1, at(p, 1, 0, 0), B2 + 8)
    for p in range(3):
        finish(p, 0, at(p, 2, 0, 0), B1)
        start_full(p, 1, at(p, 2, 0, 0), B2 + 12)
        start_full(p, 2, at(p, None, 0, 0), B3)
    for q in range(4):
        for p in range(3):
            relay(p, 1, at(p, OFFS[q], -1, 0), at(p, OFFS[q], 1, 0), B2 + 4 * q)
    for p in range(3):
        start_full(p, 2, at(p, None, -1, 0), B3 + 4)
        start_full(p, 2, at(p, None, 1, 0), B3 + 8)
    for q in range(4):
        for p in range(3):
            finish(p, 1, at(p, OFFS[q], 2, 0), B2 + 4 * q)
    for p in range(3):
        start_full(p, 2, at(p, None, 2, 0), B3 + 12)
    for q in range(4):
        for p in range(3):
            relay(p, 2, at(p, None, OFFS[q], -1), at(p, None, OFFS[q], 1), B3 + 4 * q)
    for q in range(4):
        for p in range(3):
            finish(p, 2, at(p, None, OFFS[q], 2), B3 + 4 * q)
    return descs


def block_index(b):
    return b // (SIDE * SIDE), (b // SIDE) % SIDE, b % SIDE


def hmc_kernel(step_size, solo, x_ref, start_ref, all_ref, x_all, xt_all, y_all, z_all, w2_ref, wbd_ref, a0, a1, zp0, zp1,
               b0, b1, g_ref, pos_ref, vel_ref, snd, rcv, x_send, x_recv, o_send, o_recv, e_send, e_recv, s_send, s_recv, own_sem):
    half_step = 0.5 * step_size
    me = lax.axis_index('data')
    core = me % 2
    chip = me // 2
    coords = (chip // (SIDE * SIDE), (chip // SIDE) % SIDE, chip % SIDE)
    partner = me + 1 - 2 * core

    def device_at(c):
        return ((c[0] * SIDE + c[1]) * SIDE + c[2]) * 2 + core

    own = pltpu.make_async_copy(x_ref, x_all.at[coords[0], coords[1], coords[2]], own_sem)
    own.start()
    if not solo:
        barrier = pltpu.get_barrier_semaphore()
        for axis in range(3):
            for step in (1, -1):
                to = list(coords)
                to[axis] = lax.rem(to[axis] + step + SIDE, SIDE)
                pl.semaphore_signal(barrier, inc=1, device_id={'data': device_at(to)}, device_id_type=pl.DeviceIdType.MESH)
        pl.semaphore_signal(barrier, inc=1, device_id={'data': partner}, device_id_type=pl.DeviceIdType.MESH)
        pl.semaphore_wait(barrier, 7)
    own.wait()
    if not solo:
        x_descs = torus_gather(x_all, ROW_PIECES, coords, device_at, x_send, x_recv)
        for d in x_descs:
            d.wait_send()

    def turn(b, carry):
        z, y, x = block_index(b)
        xt = x_all[z, y, x].T
        xt_all[b] = xt
        row = xt[112:128, :].astype(jnp.float32)[LAB - 112:LAB - 111, :]
        for k in range(8):
            y_all[b, k:k + 1, :] = row[:, k * LANES:(k + 1) * LANES]
        return carry

    lax.fori_loop(0, BLOCKS, turn, 0)

    pos_ref[...] = start_ref[0]
    vel_ref[...] = start_ref[1]
    lane = lax.broadcasted_iota(jnp.int32, (HID, LANES), 1)
    sub = lax.broadcasted_iota(jnp.int32, (HID, LANES), 0)
    is_param = (lane < LAB) | (lane == OUT)

    def forward(b, a_ref, zp_ref):
        xt = xt_all[b]
        pre = jnp.dot(wbd_ref[...], jnp.concatenate([xt[:, :512], xt[:, 512:]], axis=0), preferred_element_type=jnp.float32)
        act = jnp.tanh(pre)
        a_ref[...] = act
        w2 = w2_ref[...].reshape(HID // 8, 8, LANES)
        for k in range(8):
            s, j = k // 4, k % 4
            part = act[s * HID:(s + 1) * HID, j * LANES:(j + 1) * LANES].reshape(HID // 8, 8, LANES)
            zp_ref[8 * k:8 * k + 8, :] = jnp.sum(part * w2, axis=0)

    def backward(b, a_ref, zp_ref, b_ref, acc):
        z = zp_ref[pl.ds(0, 8, stride=8), :]
        for k in range(1, 8):
            z = z + zp_ref[pl.ds(k, 8, stride=8), :]
        z_all[b] = z
        res = y_all[b] - 1.0 / (1.0 + jnp.exp(-z))
        w2 = w2_ref[...]
        for j in range(4):
            parts = []
            for s in range(2):
                r = jnp.broadcast_to(res[4 * s + j:4 * s + j + 1, :], (HID, LANES))
                act = a_ref[s * HID:(s + 1) * HID, j * LANES:(j + 1) * LANES]
                ra = r * act
                acc = acc + ra
                parts.append((r - ra * act) * w2)
            b_ref[:, j * LANES:(j + 1) * LANES] = jnp.concatenate(parts, axis=0).astype(jnp.bfloat16)
        return acc

    def weight_grad(b, b_ref):
        z, y, x = block_index(b)
        rows = x_all[z, y, x]
        g_ref[...] += jnp.dot(b_ref[...], jnp.concatenate([rows[:512], rows[512:]], axis=1), preferred_element_type=jnp.float32)

    def leap(k, carry):
        pos = pos_ref[...] + jnp.where(k > 0, step_size, 0.0) * vel_ref[...]
        pos_ref[...] = pos
        w_in = jnp.where(lane < LAB, pos, 0.0)
        nil = jnp.zeros_like(w_in)
        wbd_ref[...] = jnp.concatenate([jnp.concatenate([w_in, nil], axis=1), jnp.concatenate([nil, w_in], axis=1)], axis=0).astype(jnp.bfloat16)
        w2_ref[...] = jnp.broadcast_to(pos[:, OUT:OUT + 1], (HID, LANES))
        g_ref[...] = jnp.zeros_like(g_ref)
        b1[...] = jnp.zeros_like(b1)
        forward(0, a0, zp0)

        def pair(i, acc):
            forward(2 * i + 1, a1, zp1)
            acc = backward(2 * i, a0, zp0, b0, acc)
            weight_grad(jnp.maximum(2 * i - 1, 0), b1)
            forward(jnp.minimum(2 * i + 2, BLOCKS - 1), a0, zp0)
            acc = backward(2 * i + 1, a1, zp1, b1, acc)
            weight_grad(2 * i, b0)
            return acc

        acc = lax.fori_loop(0, BLOCKS // 2, pair, jnp.zeros((HID, LANES), jnp.float32))
        weight_grad(BLOCKS - 1, b1)
        grad = g_ref[:HID, :LANES] + g_ref[HID:, LANES:]
        grad = jnp.where(lane < LAB, grad, jnp.where(lane == OUT, jnp.sum(acc, axis=1, keepdims=True), 0.0))
        slot = k % 2
        snd[slot] = grad

        @pl.when(k == LEAPS)
        def _():
            def loss_block(b, total):
                z = z_all[b]
                return total + (jnp.maximum(z, 0.0) + jnp.log1p(jnp.exp(-jnp.abs(z))) - y_all[b] * z)

            total = lax.fori_loop(0, BLOCKS, loss_block, jnp.zeros((8, LANES), jnp.float32))
            total = jnp.sum(jnp.sum(total, axis=1, keepdims=True), axis=0, keepdims=True)
            snd[slot] = jnp.where((lane == LOSS) & (sub == 0), total, grad)

        if not solo:
            ex = pltpu.make_async_remote_copy(
                src_ref=snd.at[slot], dst_ref=rcv.at[slot], send_sem=e_send, recv_sem=e_recv.at[slot],
                device_id={'data': partner}, device_id_type=pl.DeviceIdType.MESH)
            ex.start()
            ex.wait()
        total = snd[slot] + rcv[slot]
        rate = jnp.where((k == 0) | (k == LEAPS), half_step, step_size)
        vel_ref[...] += rate * jnp.where(is_param, total - pos * (1.0 / PRIOR_VAR), 0.0)
        return carry

    lax.fori_loop(0, LEAPS + 1, leap, 0)

    last = LEAPS % 2
    loss = snd[last][:1, LOSS:LOSS + 1] + rcv[last][:1, LOSS:LOSS + 1]
    pos = pos_ref[...]
    vel = vel_ref[...]
    square = (pos * pos) * (1.0 / (2.0 * PRIOR_VAR)) + 0.5 * (vel * vel)
    energy = loss + jnp.sum(jnp.sum(square, axis=1, keepdims=True), axis=0, keepdims=True)
    pos_out = jnp.where((lane == LOSS) & (sub == 0), energy, pos)
    if solo:
        all_ref[0, 0, 0, 0] = pos_out
        all_ref[1, 0, 0, 0] = vel
        return
    all_ref[core, coords[0], coords[1], coords[2]] = jnp.where(core == 0, pos_out, vel)
    o_descs = torus_gather(all_ref.at[core], OUT_PIECES, coords, device_at, o_send, o_recv)
    swap = pltpu.make_async_remote_copy(
        src_ref=all_ref.at[core], dst_ref=all_ref.at[core], send_sem=s_send, recv_sem=s_recv,
        device_id={'data': partner}, device_id_type=pl.DeviceIdType.MESH)
    swap.start()
    for d in o_descs:
        d.wait_send()
    swap.wait_send()
    pltpu.make_async_remote_copy(
        src_ref=all_ref.at[1 - core], dst_ref=all_ref.at[1 - core], send_sem=s_send, recv_sem=s_recv,
        device_id={'data': partner}, device_id_type=pl.DeviceIdType.MESH).wait_recv()


def call_kernel(x_pad, start, step_size, solo=False):
    rows = x_pad.shape[0]
    f32, bf16 = jnp.float32, jnp.bfloat16
    dma = pltpu.SemaphoreType.DMA
    return pl.pallas_call(
        functools.partial(hmc_kernel, step_size, solo),
        out_shape=jax.ShapeDtypeStruct((2, SIDE, SIDE, SIDE, HID, LANES), f32),
        in_specs=[pl.BlockSpec(memory_space=pl.ANY), pl.BlockSpec(memory_space=pltpu.VMEM)],
        out_specs=pl.BlockSpec(memory_space=pltpu.VMEM),
        scratch_shapes=[
            pltpu.VMEM((SIDE, SIDE, SIDE, rows, LANES), bf16),
            pltpu.VMEM((BLOCKS, LANES, rows), bf16),
            pltpu.VMEM((BLOCKS, 8, LANES), f32),
            pltpu.VMEM((BLOCKS, 8, LANES), f32),
            pltpu.VMEM((HID, LANES), f32),
            pltpu.VMEM((2 * HID, 2 * LANES), bf16),
            pltpu.VMEM((2 * HID, 512), f32),
            pltpu.VMEM((2 * HID, 512), f32),
            pltpu.VMEM((64, LANES), f32),
            pltpu.VMEM((64, LANES), f32),
            pltpu.VMEM((2 * HID, 512), bf16),
            pltpu.VMEM((2 * HID, 512), bf16),
            pltpu.VMEM((2 * HID, 2 * LANES), f32),
            pltpu.VMEM((HID, LANES), f32),
            pltpu.VMEM((HID, LANES), f32),
            pltpu.VMEM((2, HID, LANES), f32),
            pltpu.VMEM((2, HID, LANES), f32),
            dma((3, 36)), dma((3, 36)), dma((3, 36)), dma((3, 36)), dma, dma((2,)), dma, dma, dma,
        ],
        compiler_params=pltpu.CompilerParams(
            vmem_limit_bytes=60 * 2 ** 20, **({} if solo else dict(collective_id=0, has_side_effects=True))),
        name='hmc',
    )(x_pad, start)


def solution(mesh):
    row_spec = P('data', None)
    label_spec = P('data')
    in_spec = P(None, 'parts', None)
    out_spec = P('parts', None)
    chain_spec = P('parts')

    def run_chains(feats, labels, w_in, w_out, mom_in, mom_out):
        num_rows, num_feat = feats.shape
        hidden = w_in.shape[2]
        step_size = 1.0 / math.sqrt(num_rows * (num_feat + hidden))

        def device_body(x_rows, y_rows, pos_in, pos_out, vel_in, vel_out):
            x_pad = jnp.concatenate([x_rows, y_rows.astype(jnp.bfloat16)[:, None]], axis=1)
            x_pad = jnp.pad(x_pad, ((0, 0), (0, LANES - num_feat - 1)))
            chain = lax.axis_index('data') // 2

            def pack(arr_in, arr_out):
                mine_in = lax.dynamic_slice_in_dim(arr_in, chain, 1, axis=1)[:, 0, :]
                mine_out = lax.dynamic_slice_in_dim(arr_out, chain, 1, axis=0)
                both = jnp.concatenate([mine_in, jnp.zeros((OUT - num_feat, hidden), jnp.float32), mine_out], axis=0)
                return jnp.pad(both.T, ((0, HID - hidden), (0, 0)))

            start = jnp.stack([pack(pos_in, pos_out), pack(vel_in, vel_out)])
            every = call_kernel(x_pad, start, step_size).reshape(2, BLOCKS, HID, LANES)
            whole = jnp.transpose(every[:, :, :hidden, :], (0, 3, 1, 2))
            return (whole[0, :num_feat], whole[0, OUT], whole[1, :num_feat], whole[1, OUT], every[0, :, 0, LOSS])

        mapped = jax.shard_map(device_body, mesh=mesh, in_specs=(row_spec, label_spec, in_spec, out_spec, in_spec, out_spec), out_specs=(in_spec, out_spec, in_spec, out_spec, chain_spec), check_vma=False)
        return mapped(feats, labels, w_in, w_out, mom_in, mom_out)

    return run_chains
```

```python
import functools
import math

import jax
import jax.numpy as jnp
from jax import lax
from jax.experimental import pallas as pl
from jax.experimental.pallas import tpu as pltpu
from jax.sharding import PartitionSpec as P

LEAPS = 16
PRIOR_VAR = 1.0
SIDE = 4
BLOCKS = SIDE ** 3
HID = 56
LANES = 128
LAB = 123
LOSS = 124
OUT = 127
UNIT = 8
ROW_PIECES = ((0, 352, 176), (352, 336, 176), (688, 336, 176))
OUT_PIECES = ((0, 24, 16), (24, 16, 8), (40, 16, 8))


def torus_gather(buf, pieces, coords, device_at, send_sem, recv_sem, near=None, middle=None):
    descs = []
    plus = lambda c, d: lax.rem(c + d + SIDE, SIDE)

    def view(p, where, part):
        start, size, first = pieces[p]
        lo, n = {0: (start, size), 1: (start, first), 2: (start + first, size - first)}[part]
        return buf.at[where[0], where[1], where[2], pl.ds(lo, n), :]

    def copy(p, where, part, axis, step, slot):
        to = list(coords)
        to[axis] = plus(to[axis], step)
        ref = view(p, where, part)
        return pltpu.make_async_remote_copy(
            src_ref=ref, dst_ref=ref, send_sem=send_sem.at[p, slot], recv_sem=recv_sem.at[p, slot],
            device_id={'data': device_at(to)}, device_id_type=pl.DeviceIdType.MESH)

    def send(p, where, part, axis, step, slot):
        c = copy(p, where, part, axis, step, slot)
        c.start()
        descs.append(c)

    def wait(p, where, part, axis, step, slot):
        copy(p, where, part, axis, step, slot).wait_recv()

    orders = [(p, (p + 1) % 3, (p + 2) % 3) for p in range(3)]
    OFFS = (0, -1, 1, 2)

    def at(p, off0, off1, off2):
        where = [None, None, None]
        for axis, off in zip(orders[p], (off0, off1, off2)):
            where[axis] = slice(None) if off is None else (coords[axis] if off == 0 else plus(coords[axis], off))
        return where

    def start_full(p, ph, own, base):
        axis = orders[p][ph]
        send(p, own, 0, axis, 1, base)
        send(p, own, 0, axis, -1, base + 1)

    def relay(p, ph, low, high, base):
        axis = orders[p][ph]
        wait(p, low, 0, axis, 1, base)
        send(p, low, 1, axis, 1, base + 2)
        wait(p, high, 0, axis, 1, base + 1)
        send(p, high, 2, axis, -1, base + 3)

    def finish(p, ph, far, base):
        axis = orders[p][ph]
        wait(p, far, 1, axis, 1, base + 2)
        wait(p, far, 2, axis, 1, base + 3)

    B1, B2, B3 = 0, 4, 20
    for p in range(3):
        start_full(p, 0, at(p, 0, 0, 0), B1)
    for p in range(3):
        start_full(p, 1, at(p, 0, 0, 0), B2)
    for p in range(3):
        relay(p, 0, at(p, -1, 0, 0), at(p, 1, 0, 0), B1)
        start_full(p, 1, at(p, -1, 0, 0), B2 + 4)
        start_full(p, 1, at(p, 1, 0, 0), B2 + 8)
    for p in range(3):
        finish(p, 0, at(p, 2, 0, 0), B1)
        start_full(p, 1, at(p, 2, 0, 0), B2 + 12)
        start_full(p, 2, at(p, None, 0, 0), B3)
    for q in range(4):
        for p in range(3):
            relay(p, 1, at(p, OFFS[q], -1, 0), at(p, OFFS[q], 1, 0), B2 + 4 * q)
    for p in range(3):
        start_full(p, 2, at(p, None, -1, 0), B3 + 4)
        start_full(p, 2, at(p, None, 1, 0), B3 + 8)
    for q in range(4):
        for p in range(3):
            finish(p, 1, at(p, OFFS[q], 2, 0), B2 + 4 * q)
    for p in range(3):
        start_full(p, 2, at(p, None, 2, 0), B3 + 12)
    for q in range(4):
        for p in range(3):
            relay(p, 2, at(p, None, OFFS[q], -1), at(p, None, OFFS[q], 1), B3 + 4 * q)
    if near is not None:
        near()
    for q in range(4):
        if q == 3 and middle is not None:
            middle()
        for p in range(3):
            finish(p, 2, at(p, None, OFFS[q], 2), B3 + 4 * q)
    return descs


def block_index(b):
    return b // (SIDE * SIDE), (b // SIDE) % SIDE, b % SIDE


def hmc_kernel(step_size, solo, feat_ref, lab_ref, w_ref, wo_ref, m_ref, mo_ref, w_end, wo_end, m_end, mo_end, e_end,
               x_in, w_tmp, x_all, xt_all, y_all, z_all, w2_ref, wbd_ref, a_ref, zp_ref,
               b_ref, g_ref, pos_ref, vel_ref, snd, rcv, all_ref, x_send, x_recv, o_send, o_recv, e_send, e_recv, s_send, s_recv, own_sem):
    half_step = 0.5 * step_size
    num_feat = feat_ref.shape[1]
    hidden = w_ref.shape[0]
    me = lax.axis_index('data')
    core = me % 2
    chip = me // 2
    coords = (chip // (SIDE * SIDE), (chip // SIDE) % SIDE, chip % SIDE)
    partner = me + 1 - 2 * core

    def device_at(c):
        return ((c[0] * SIDE + c[1]) * SIDE + c[2]) * 2 + core

    loads = [pltpu.make_async_copy(feat_ref, x_in, own_sem.at[0])]
    eight = pl.multiple_of((chip // 8) * 8, 8)
    for n, ref in enumerate((w_ref, m_ref)):
        loads.append(pltpu.make_async_copy(ref.at[:, pl.ds(eight, 8), :], w_tmp.at[n], own_sem.at[n + 1]))
    for load in loads:
        load.start()
    if not solo:
        barrier = pltpu.get_barrier_semaphore()
        for axis in range(3):
            for step in (1, -1):
                to = list(coords)
                to[axis] = lax.rem(to[axis] + step + SIDE, SIDE)
                pl.semaphore_signal(barrier, inc=1, device_id={'data': device_at(to)}, device_id_type=pl.DeviceIdType.MESH)
        pl.semaphore_signal(barrier, inc=1, device_id={'data': partner}, device_id_type=pl.DeviceIdType.MESH)
    labels = lab_ref[...].astype(jnp.float32)
    loads[0].wait()
    for k in range(8):
        column = jnp.broadcast_to(labels[k:k + 1, :], (LANES, LANES)).T
        spare = lax.broadcasted_iota(jnp.int32, (LANES, LANES), 1)
        rows = pl.ds(k * LANES, LANES)
        x_all[coords[0], coords[1], coords[2], rows, :] = jnp.where(spare == LAB, column, 0.0).astype(jnp.bfloat16)
        x_all[coords[0], coords[1], coords[2], rows, :num_feat] = x_in[rows, :]
    if not solo:
        pl.semaphore_wait(barrier, 7)

    def turn(where):
        z, y, x = where
        b = (z * SIDE + y) * SIDE + x
        for k in range(8):
            xt = x_all[z, y, x, k * LANES:(k + 1) * LANES, :].T
            xt_all[b, k] = xt
            y_all[b, k:k + 1, :] = xt[112:128, :].astype(jnp.float32)[LAB - 112:LAB - 111, :]

    def moved(offsets):
        return tuple(lax.rem(c + o, SIDE) for c, o in zip(coords, offsets))

    def three(i):
        return 3 + i

    def near():
        def body(i, carry):
            turn(moved((three(i // 9), three((i // 3) % 3), three(i % 3))))
            return carry
        lax.fori_loop(0, 27, body, 0)

    def middle():
        def body(i, carry):
            u, v = three(i // 3), three(i % 3)
            turn(moved((2, u, v)))
            turn(moved((u, 2, v)))
            turn(moved((u, v, 2)))
            return carry
        lax.fori_loop(0, 9, body, 0)

    def far():
        def body(i, carry):
            u = three(i)
            turn(moved((2, 2, u)))
            turn(moved((2, u, 2)))
            turn(moved((u, 2, 2)))
            return carry
        lax.fori_loop(0, 3, body, 0)
        turn(moved((2, 2, 2)))

    x_descs = []
    if solo:
        near()
        middle()
    else:
        x_descs = torus_gather(x_all, ROW_PIECES, coords, device_at, x_send, x_recv, near, middle)
    far()
    for d in x_descs:
        d.wait_send()
    pos_ref[...] = jnp.zeros_like(pos_ref)
    vel_ref[...] = jnp.zeros_like(vel_ref)
    chain_row = lax.broadcasted_iota(jnp.int32, (hidden, 8, num_feat), 1) == chip % 8
    chain_lane = lax.broadcasted_iota(jnp.int32, wo_ref.shape, 1) == chip
    for n, (ref, last) in enumerate(((pos_ref, wo_ref), (vel_ref, mo_ref))):
        loads[n + 1].wait()
        ref[:hidden, :num_feat] = jnp.sum(jnp.where(chain_row, w_tmp[n], 0.0), axis=1)
        ref[:hidden, OUT:OUT + 1] = jnp.sum(jnp.where(chain_lane, last[...], 0.0), axis=1, keepdims=True)

    lane = lax.broadcasted_iota(jnp.int32, (HID, LANES), 1)
    sub = lax.broadcasted_iota(jnp.int32, (HID, LANES), 0)
    is_param = (lane < LAB) | (lane == OUT)

    def forward(b):
        wbd = jnp.concatenate([wbd_ref[0], wbd_ref[1]], axis=1)
        pres = []
        for t in range(2):
            tiles = [jnp.concatenate([xt_all[b, 4 * s + 2 * t], xt_all[b, 4 * s + 2 * t + 1]], axis=1) for s in range(2)]
            pres.append(jnp.dot(wbd, jnp.concatenate(tiles, axis=0), preferred_element_type=jnp.float32))
        return pres

    def activate(pres, u):
        w2 = w2_ref[...].reshape(HID // 8, 8, LANES)
        for t in range(2):
            act = jnp.tanh(pres[t])
            for h in range(2):
                j = 2 * t + h
                a_ref[u, j] = act[:, h * LANES:(h + 1) * LANES]
                for s in range(2):
                    part = act[s * HID:(s + 1) * HID, h * LANES:(h + 1) * LANES].reshape(HID // 8, 8, LANES)
                    k = 4 * s + j
                    zp_ref[u, 8 * k:8 * k + 8, :] = jnp.sum(part * w2, axis=0)

    def backward(b, u, acc):
        z = zp_ref[u, pl.ds(0, 8, stride=8), :]
        for k in range(1, 8):
            z = z + zp_ref[u, pl.ds(k, 8, stride=8), :]
        z_all[b] = z
        res = y_all[b] - 1.0 / (1.0 + jnp.exp(-z))
        w2 = w2_ref[...]
        for j in range(4):
            parts = []
            for s in range(2):
                r = jnp.broadcast_to(res[4 * s + j:4 * s + j + 1, :], (HID, LANES))
                act = a_ref[u, j, s * HID:(s + 1) * HID, :]
                ra = r * act
                acc = acc + ra
                parts.append((r - ra * act) * w2)
            b_ref[u, j] = jnp.concatenate(parts, axis=0).astype(jnp.bfloat16)
        return acc

    def weight_grad(b, u):
        z, y, x = block_index(b)
        rows = x_all.at[z, y, x]
        lhs = jnp.concatenate([b_ref[u, j] for j in range(4)], axis=1)
        return jnp.dot(lhs, jnp.concatenate([rows[:512, :], rows[512:, :]], axis=1), preferred_element_type=jnp.float32)

    def leap(k, carry):
        pos = pos_ref[...] + jnp.where(k > 0, step_size, 0.0) * vel_ref[...]
        pos_ref[...] = pos
        w_in = jnp.where(lane < LAB, pos, 0.0)
        nil = jnp.zeros_like(w_in)
        wbd_ref[0] = jnp.concatenate([w_in, nil], axis=0).astype(jnp.bfloat16)
        wbd_ref[1] = jnp.concatenate([nil, w_in], axis=0).astype(jnp.bfloat16)
        w2_ref[...] = jnp.broadcast_to(pos[:, OUT:OUT + 1], (HID, LANES))
        g_ref[...] = jnp.zeros_like(g_ref)
        b_ref[...] = jnp.zeros_like(b_ref)
        for u in range(UNIT):
            activate(forward(u), u)

        def unit(i, acc):
            now = i * UNIT
            prior = jnp.maximum(now - UNIT, 0)
            ahead = jnp.minimum(now + UNIT, BLOCKS - UNIT)
            pres = [forward(ahead + u) for u in range(UNIT)]
            part = weight_grad(prior, 0)
            for u in range(1, UNIT):
                part = part + weight_grad(prior + u, u)
            for u in range(UNIT):
                acc = backward(now + u, u, acc)
            for u in range(UNIT):
                activate(pres[u], u)
            g_ref[...] += part
            return acc

        acc = lax.fori_loop(0, BLOCKS // UNIT, unit, jnp.zeros((HID, LANES), jnp.float32))
        for u in range(UNIT):
            g_ref[...] += weight_grad(BLOCKS - UNIT + u, u)
        grad = g_ref[:HID, :LANES] + g_ref[HID:, LANES:]
        grad = jnp.where(lane < LAB, grad, jnp.where(lane == OUT, jnp.sum(acc, axis=1, keepdims=True), 0.0))
        slot = k % 2
        snd[slot] = grad

        @pl.when(k == LEAPS)
        def _():
            def loss_block(b, total):
                z = z_all[b]
                return total + (jnp.maximum(z, 0.0) + jnp.log1p(jnp.exp(-jnp.abs(z))) - y_all[b] * z)

            total = lax.fori_loop(0, BLOCKS, loss_block, jnp.zeros((8, LANES), jnp.float32))
            total = jnp.sum(jnp.sum(total, axis=1, keepdims=True), axis=0, keepdims=True)
            snd[slot] = jnp.where((lane == LOSS) & (sub == 0), total, grad)

        if not solo:
            ex = pltpu.make_async_remote_copy(
                src_ref=snd.at[slot], dst_ref=rcv.at[slot], send_sem=e_send, recv_sem=e_recv.at[slot],
                device_id={'data': partner}, device_id_type=pl.DeviceIdType.MESH)
            ex.start()
            ex.wait()
        total = snd[slot] + rcv[slot]
        rate = jnp.where((k == 0) | (k == LEAPS), half_step, step_size)
        vel_ref[...] += rate * jnp.where(is_param, total - pos * (1.0 / PRIOR_VAR), 0.0)
        return carry

    lax.fori_loop(0, LEAPS + 1, leap, 0)

    last = LEAPS % 2
    loss = snd[last][:1, LOSS:LOSS + 1] + rcv[last][:1, LOSS:LOSS + 1]
    pos = pos_ref[...]
    vel = vel_ref[...]
    square = (pos * pos) * (1.0 / (2.0 * PRIOR_VAR)) + 0.5 * (vel * vel)
    energy = loss + jnp.sum(jnp.sum(square, axis=1, keepdims=True), axis=0, keepdims=True)
    tails = []
    for ref in (pos_ref, vel_ref):
        w2 = jnp.broadcast_to(ref[...][:, OUT:OUT + 1], (HID, LANES))
        row = jnp.concatenate([w2, jnp.zeros((LANES - HID, LANES), jnp.float32)], axis=0).T[:1, :]
        tails.append(jnp.broadcast_to(row, (HID, LANES)))
    tails[0] = jnp.where(lane == hidden, energy, tails[0])
    outs = [jnp.where(sub == hidden, t, v) for t, v in zip(tails, (pos, vel))]
    if solo:
        all_ref[0, 0, 0, 0] = outs[0]
        all_ref[1, 0, 0, 0] = outs[1]
    else:
        all_ref[core, coords[0], coords[1], coords[2]] = jnp.where(core == 0, outs[0], outs[1])
        o_descs = torus_gather(all_ref.at[core], OUT_PIECES, coords, device_at, o_send, o_recv)
        swap = pltpu.make_async_remote_copy(
            src_ref=all_ref.at[core], dst_ref=all_ref.at[core], send_sem=s_send, recv_sem=s_recv,
            device_id={'data': partner}, device_id_type=pl.DeviceIdType.MESH)
        swap.start()
        for d in o_descs:
            d.wait_send()
        swap.wait_send()
        pltpu.make_async_remote_copy(
            src_ref=all_ref.at[1 - core], dst_ref=all_ref.at[1 - core], send_sem=s_send, recv_sem=s_recv,
            device_id={'data': partner}, device_id_type=pl.DeviceIdType.MESH).wait_recv()

    flat = all_ref.reshape(2, BLOCKS * HID, LANES)

    def spread(h, carry):
        for n, ref in enumerate((w_end, m_end)):
            for c in range(0, BLOCKS, 8):
                ref[h, c:c + 8, :] = flat[n, pl.ds(c * HID + h, 8, stride=HID), :][:, :num_feat]
        return carry

    lax.fori_loop(0, hidden, spread, 0)
    for n, ref in enumerate((wo_end, mo_end)):
        tail = jnp.concatenate([flat[n, pl.ds(c * HID + hidden, 8, stride=HID), :] for c in range(0, BLOCKS, 8)]
                               + [jnp.zeros((LANES - BLOCKS, LANES), jnp.float32)], axis=0).T
        ref[...] = tail[:hidden, :BLOCKS]
        if n == 0:
            e_end[...] = tail[hidden:hidden + 1, :BLOCKS]


def call_kernel(feats, labels, w_in, w_out, mom_in, mom_out, step_size, solo=False):
    rows, num_feat = feats.shape
    hidden, chains, _ = w_in.shape
    f32, bf16 = jnp.float32, jnp.bfloat16
    dma = pltpu.SemaphoreType.DMA
    vmem = pl.BlockSpec(memory_space=pltpu.VMEM)
    hbm = pl.BlockSpec(memory_space=pl.ANY)
    return pl.pallas_call(
        functools.partial(hmc_kernel, step_size, solo),
        out_shape=[jax.ShapeDtypeStruct(w_in.shape, f32), jax.ShapeDtypeStruct(w_out.shape, f32)] * 2 + [jax.ShapeDtypeStruct((1, chains), f32)],
        in_specs=[hbm, vmem, hbm, vmem, hbm, vmem],
        out_specs=[vmem] * 5,
        scratch_shapes=[
            pltpu.VMEM((rows, num_feat), bf16),
            pltpu.VMEM((2, hidden, 8, num_feat), f32),
            pltpu.VMEM((SIDE, SIDE, SIDE, rows, LANES), bf16),
            pltpu.VMEM((BLOCKS, rows // LANES, LANES, LANES), bf16),
            pltpu.VMEM((BLOCKS, 8, LANES), f32),
            pltpu.VMEM((BLOCKS, 8, LANES), f32),
            pltpu.VMEM((HID, LANES), f32),
            pltpu.VMEM((2, 2 * HID, LANES), bf16),
            pltpu.VMEM((UNIT, 4, 2 * HID, LANES), f32),
            pltpu.VMEM((UNIT, 64, LANES), f32),
            pltpu.VMEM((UNIT, 4, 2 * HID, LANES), bf16),
            pltpu.VMEM((2 * HID, 2 * LANES), f32),
            pltpu.VMEM((HID, LANES), f32),
            pltpu.VMEM((HID, LANES), f32),
            pltpu.VMEM((2, HID, LANES), f32),
            pltpu.VMEM((2, HID, LANES), f32),
            pltpu.VMEM((2, SIDE, SIDE, SIDE, HID, LANES), f32),
            dma((3, 36)), dma((3, 36)), dma((3, 36)), dma((3, 36)), dma, dma((2,)), dma, dma, dma((3,)),
        ],
        compiler_params=pltpu.CompilerParams(
            vmem_limit_bytes=60 * 2 ** 20, **({} if solo else dict(collective_id=0, has_side_effects=True))),
        name='hmc',
    )(feats, labels, w_in, w_out, mom_in, mom_out)


def solution(mesh):
    row_spec = P('data', None)
    label_spec = P('data')
    in_spec = P(None, 'parts', None)
    out_spec = P('parts', None)
    chain_spec = P('parts')

    def run_chains(feats, labels, w_in, w_out, mom_in, mom_out):
        num_rows, num_feat = feats.shape
        hidden = w_in.shape[2]
        step_size = 1.0 / math.sqrt(num_rows * (num_feat + hidden))

        def device_body(x_rows, y_rows, pos_in, pos_out, vel_in, vel_out):
            turned = [jnp.transpose(v) for v in (pos_in, pos_out, vel_in, vel_out)]
            ends = call_kernel(x_rows, y_rows.reshape(8, LANES), *turned, step_size)
            return tuple(jnp.transpose(v) for v in ends[:4]) + (ends[4].reshape(-1),)

        mapped = jax.shard_map(device_body, mesh=mesh, in_specs=(row_spec, label_spec, in_spec, out_spec, in_spec, out_spec), out_specs=(in_spec, out_spec, in_spec, out_spec, chain_spec), check_vma=False)
        return mapped(feats, labels, w_in, w_out, mom_in, mom_out)

    return run_chains
```

```python
import functools
import math

import jax
import jax.numpy as jnp
from jax import lax
from jax.experimental import pallas as pl
from jax.experimental.pallas import tpu as pltpu
from jax.sharding import PartitionSpec as P

LEAPS = 16
PRIOR_VAR = 1.0
SIDE = 4
BLOCKS = SIDE ** 3
HID = 56
LANES = 128
LAB = 123
LOSS = 124
OUT = 127
UNROLL = 4
MIB = 2 ** 20
ROW_PIECES = ((0, 352, 176), (352, 336, 176), (688, 336, 176))
OUT_PIECES = ((0, 24, 16), (24, 16, 8), (40, 16, 8))


def torus_gather(buf, pieces, coords, device_at, send_sem, recv_sem, near=None, middle=None):
    descs = []
    plus = lambda c, d: lax.rem(c + d + SIDE, SIDE)

    def view(p, where, part):
        start, size, first = pieces[p]
        lo, n = {0: (start, size), 1: (start, first), 2: (start + first, size - first)}[part]
        return buf.at[where[0], where[1], where[2], pl.ds(lo, n), :]

    def copy(p, where, part, axis, step, slot):
        to = list(coords)
        to[axis] = plus(to[axis], step)
        ref = view(p, where, part)
        return pltpu.make_async_remote_copy(
            src_ref=ref, dst_ref=ref, send_sem=send_sem.at[p, slot], recv_sem=recv_sem.at[p, slot],
            device_id={'data': device_at(to)}, device_id_type=pl.DeviceIdType.MESH)

    def send(p, where, part, axis, step, slot):
        c = copy(p, where, part, axis, step, slot)
        c.start()
        descs.append(c)

    def wait(p, where, part, axis, step, slot):
        copy(p, where, part, axis, step, slot).wait_recv()

    orders = [(p, (p + 1) % 3, (p + 2) % 3) for p in range(3)]
    OFFS = (0, -1, 1, 2)

    def at(p, off0, off1, off2):
        where = [None, None, None]
        for axis, off in zip(orders[p], (off0, off1, off2)):
            where[axis] = slice(None) if off is None else (coords[axis] if off == 0 else plus(coords[axis], off))
        return where

    def start_full(p, ph, own, base):
        axis = orders[p][ph]
        send(p, own, 0, axis, 1, base)
        send(p, own, 0, axis, -1, base + 1)

    def relay(p, ph, low, high, base):
        axis = orders[p][ph]
        wait(p, low, 0, axis, 1, base)
        send(p, low, 1, axis, 1, base + 2)
        wait(p, high, 0, axis, 1, base + 1)
        send(p, high, 2, axis, -1, base + 3)

    def finish(p, ph, far, base):
        axis = orders[p][ph]
        wait(p, far, 1, axis, 1, base + 2)
        wait(p, far, 2, axis, 1, base + 3)

    B1, B2, B3 = 0, 4, 20
    for p in range(3):
        start_full(p, 0, at(p, 0, 0, 0), B1)
    for p in range(3):
        start_full(p, 1, at(p, 0, 0, 0), B2)
    for p in range(3):
        relay(p, 0, at(p, -1, 0, 0), at(p, 1, 0, 0), B1)
        start_full(p, 1, at(p, -1, 0, 0), B2 + 4)
        start_full(p, 1, at(p, 1, 0, 0), B2 + 8)
    for p in range(3):
        finish(p, 0, at(p, 2, 0, 0), B1)
        start_full(p, 1, at(p, 2, 0, 0), B2 + 12)
        start_full(p, 2, at(p, None, 0, 0), B3)
    for q in range(4):
        for p in range(3):
            relay(p, 1, at(p, OFFS[q], -1, 0), at(p, OFFS[q], 1, 0), B2 + 4 * q)
    for p in range(3):
        start_full(p, 2, at(p, None, -1, 0), B3 + 4)
        start_full(p, 2, at(p, None, 1, 0), B3 + 8)
    for q in range(4):
        for p in range(3):
            finish(p, 1, at(p, OFFS[q], 2, 0), B2 + 4 * q)
    for p in range(3):
        start_full(p, 2, at(p, None, 2, 0), B3 + 12)
    for q in range(4):
        for p in range(3):
            relay(p, 2, at(p, None, OFFS[q], -1), at(p, None, OFFS[q], 1), B3 + 4 * q)
    if near is not None:
        near()
    for q in range(4):
        if q == 3 and middle is not None:
            middle()
        for p in range(3):
            finish(p, 2, at(p, None, OFFS[q], 2), B3 + 4 * q)
    return descs


def block_index(b):
    return b // (SIDE * SIDE), (b // SIDE) % SIDE, b % SIDE


def place():
    me = lax.axis_index('data')
    core = me % 2
    chip = me // 2
    coords = (chip // (SIDE * SIDE), (chip // SIDE) % SIDE, chip % SIDE)

    def device_at(c):
        return ((c[0] * SIDE + c[1]) * SIDE + c[2]) * 2 + core

    return core, chip, coords, me + 1 - 2 * core, device_at


def greet(devices):
    barrier = pltpu.get_barrier_semaphore()
    for device in devices:
        pl.semaphore_signal(barrier, inc=1, device_id={'data': device}, device_id_type=pl.DeviceIdType.MESH)
    return lambda: pl.semaphore_wait(barrier, len(devices))


def torus_neighbours(coords, device_at):
    found = []
    for axis in range(3):
        for step in (1, -1):
            to = list(coords)
            to[axis] = lax.rem(to[axis] + step + SIDE, SIDE)
            found.append(device_at(to))
    return found


def grids():
    lane = lax.broadcasted_iota(jnp.int32, (HID, LANES), 1)
    sub = lax.broadcasted_iota(jnp.int32, (HID, LANES), 0)
    return lane, sub


def collect_rows(feat_ref, lab_ref, w_ref, wo_ref, m_ref, mo_ref, x_all, xt_all, y_all, pos_ref, vel_ref,
                 x_in, w_tmp, x_send, x_recv, own_sem):
    num_feat = feat_ref.shape[1]
    hidden = w_ref.shape[0]
    core, chip, coords, partner, device_at = place()
    loads = [pltpu.make_async_copy(feat_ref, x_in, own_sem.at[0])]
    eight = pl.multiple_of((chip // 8) * 8, 8)
    for n, ref in enumerate((w_ref, m_ref)):
        loads.append(pltpu.make_async_copy(ref.at[:, pl.ds(eight, 8), :], w_tmp.at[n], own_sem.at[n + 1]))
    for load in loads:
        load.start()
    ready = greet(torus_neighbours(coords, device_at))
    labels = lab_ref[...].astype(jnp.float32)
    loads[0].wait()
    for k in range(8):
        column = jnp.broadcast_to(labels[k:k + 1, :], (LANES, LANES)).T
        spare = lax.broadcasted_iota(jnp.int32, (LANES, LANES), 1)
        rows = pl.ds(k * LANES, LANES)
        x_all[coords[0], coords[1], coords[2], rows, :] = jnp.where(spare == LAB, column, 0.0).astype(jnp.bfloat16)
        x_all[coords[0], coords[1], coords[2], rows, :num_feat] = x_in[rows, :]
    ready()

    def turn(where):
        z, y, x = where
        b = (z * SIDE + y) * SIDE + x
        for k in range(8):
            xt = x_all[z, y, x, k * LANES:(k + 1) * LANES, :].T
            xt_all[b, k] = xt
            y_all[b, k:k + 1, :] = xt[112:128, :].astype(jnp.float32)[LAB - 112:LAB - 111, :]

    def moved(offsets):
        return tuple(lax.rem(c + o, SIDE) for c, o in zip(coords, offsets))

    def three(i):
        return 3 + i

    def near():
        def body(i, carry):
            turn(moved((three(i // 9), three((i // 3) % 3), three(i % 3))))
            return carry
        lax.fori_loop(0, 27, body, 0)

    def middle():
        def body(i, carry):
            u, v = three(i // 3), three(i % 3)
            turn(moved((2, u, v)))
            turn(moved((u, 2, v)))
            turn(moved((u, v, 2)))
            return carry
        lax.fori_loop(0, 9, body, 0)

    def far():
        def body(i, carry):
            u = three(i)
            turn(moved((2, 2, u)))
            turn(moved((2, u, 2)))
            turn(moved((u, 2, 2)))
            return carry
        lax.fori_loop(0, 3, body, 0)
        turn(moved((2, 2, 2)))

    x_descs = torus_gather(x_all, ROW_PIECES, coords, device_at, x_send, x_recv, near, middle)
    far()
    for d in x_descs:
        d.wait_send()
    pos_ref[...] = jnp.zeros_like(pos_ref)
    vel_ref[...] = jnp.zeros_like(vel_ref)
    chain_row = lax.broadcasted_iota(jnp.int32, (hidden, 8, num_feat), 1) == chip % 8
    chain_lane = lax.broadcasted_iota(jnp.int32, wo_ref.shape, 1) == chip
    for n, (ref, last) in enumerate(((pos_ref, wo_ref), (vel_ref, mo_ref))):
        loads[n + 1].wait()
        ref[:hidden, :num_feat] = jnp.sum(jnp.where(chain_row, w_tmp[n], 0.0), axis=1)
        ref[:hidden, OUT:OUT + 1] = jnp.sum(jnp.where(chain_lane, last[...], 0.0), axis=1, keepdims=True)


def gradient(with_loss, *refs):
    def with_acc(pre, grad):
        gradient_body(with_loss, pre, grad, *refs)

    def spec(q):
        return pltpu.ACC(q)((2 * HID, 2 * LANES), jnp.float32)

    pl.run_scoped(with_acc, ((spec(0), spec(1)), (spec(0), spec(1))), (spec(0), spec(1)))


def gradient_body(with_loss, pre_acc, grad_acc, x_all, xt_all, y_all, pos_ref, part_ref, z_all, w2_ref, wbd_ref, b_ref):
    lane, sub = grids()
    def push_forward(b):
        for q in range(2):
            tiles = [jnp.concatenate([xt_all[b, 4 * s + 2 * q], xt_all[b, 4 * s + 2 * q + 1]], axis=1) for s in range(2)]
            pltpu.matmul_push_rhs(jnp.concatenate(tiles, axis=0), staging_register=0, mxu_index=q)

    def forward(u):
        wbd = jnp.concatenate([wbd_ref[0], wbd_ref[1]], axis=1)
        for q in range(2):
            pltpu.matmul_acc_lhs(pre_acc[u][q], wbd, load_staged_rhs=0)

    def rows_to_back(b, u, acc):
        w2 = w2_ref[...].reshape(HID // 8, 8, LANES)
        for q in range(2):
            act = jnp.tanh(pltpu.matmul_pop(pre_acc[u][q]))
            for h in range(2):
                j = 2 * q + h
                parts = []
                for s in range(2):
                    k = 4 * s + j
                    part = act[s * HID:(s + 1) * HID, h * LANES:(h + 1) * LANES].reshape(HID // 8, 8, LANES)
                    z = jnp.sum(part * w2, axis=0)
                    for shift in (4, 2, 1):
                        z = z + pltpu.roll(z, shift, 0)
                    z_all[b, k:k + 1, :] = z[:1]
                    res = jnp.broadcast_to(y_all[b, k:k + 1, :], (8, LANES)) - 1.0 / (1.0 + jnp.exp(-z))
                    weighed = part * res
                    acc = acc + weighed
                    parts.append(((res - weighed * part) * w2).reshape(HID, LANES))
                b_ref[u, j] = jnp.concatenate(parts, axis=0).astype(jnp.bfloat16)
        return acc

    def push_grad(b):
        z, y, x = block_index(b)
        rows = x_all.at[z, y, x]
        for q in range(2):
            tile = jnp.concatenate([rows[256 * q:256 * q + 256, :], rows[512 + 256 * q:768 + 256 * q, :]], axis=1)
            pltpu.matmul_push_rhs(tile, staging_register=1, mxu_index=q)

    def weight_grad(u):
        for q in range(2):
            lhs = jnp.concatenate([b_ref[u, 2 * q], b_ref[u, 2 * q + 1]], axis=1)
            pltpu.matmul_acc_lhs(grad_acc[q], lhs, load_staged_rhs=1)

    pos = pos_ref[...]
    w_in = jnp.where(lane < LAB, pos, 0.0)
    nil = jnp.zeros_like(w_in)
    wbd_ref[0] = jnp.concatenate([w_in, nil], axis=0).astype(jnp.bfloat16)
    wbd_ref[1] = jnp.concatenate([nil, w_in], axis=0).astype(jnp.bfloat16)
    w2_ref[...] = jnp.broadcast_to(pos[:, OUT:OUT + 1], (HID, LANES))
    b_ref[1] = jnp.zeros((4, 2 * HID, LANES), jnp.bfloat16)
    for u in range(2):
        push_forward(u)
        forward(u)
    push_forward(2)
    push_grad(0)

    def pair(i, acc):
        for v in range(UNROLL):
            u = v % 2
            n = UNROLL * i + v
            acc = rows_to_back(n, u, acc)
            forward(u)
            push_forward(jnp.minimum(n + 3, BLOCKS - 1))
            weight_grad(1 - u)
            push_grad(n)
        return acc

    acc = lax.fori_loop(0, BLOCKS // UNROLL, pair, jnp.zeros((HID // 8, 8, LANES), jnp.float32)).reshape(HID, LANES)
    weight_grad(1)
    for u in range(2):
        if u == 0:
            forward(u)
        for q in range(2):
            pltpu.matmul_pop(pre_acc[u][q])
    whole = pltpu.matmul_pop(grad_acc[0]) + pltpu.matmul_pop(grad_acc[1])
    grad = whole[:HID, :LANES] + whole[HID:, LANES:]
    grad = jnp.where(lane < LAB, grad, jnp.where(lane == OUT, jnp.sum(acc, axis=1, keepdims=True), 0.0))
    if with_loss:
        def loss_block(b, total):
            z = z_all[b]
            return total + (jnp.maximum(z, 0.0) + jnp.log1p(jnp.exp(-jnp.abs(z))) - y_all[b] * z)

        total = lax.fori_loop(0, BLOCKS, loss_block, jnp.zeros((8, LANES), jnp.float32))
        total = jnp.sum(jnp.sum(total, axis=1, keepdims=True), axis=0, keepdims=True)
        grad = jnp.where((lane == LOSS) & (sub == 0), total, grad)
    part_ref[...] = grad


def both_parts(part_ref, rcv, partner, e_send, e_recv):
    ex = pltpu.make_async_remote_copy(
        src_ref=part_ref, dst_ref=rcv, send_sem=e_send, recv_sem=e_recv,
        device_id={'data': partner}, device_id_type=pl.DeviceIdType.MESH)
    ex.start()
    ex.wait()
    return part_ref[...] + rcv[...]


def kick(vel, pos, total, rate):
    lane, _ = grids()
    is_param = (lane < LAB) | (lane == OUT)
    return vel + rate * jnp.where(is_param, total - pos * (1.0 / PRIOR_VAR), 0.0)


def leap(rate, step_size, part_ref, pos_ref, vel_ref, pos_new, vel_new, rcv, e_send, e_recv):
    _, _, _, partner, _ = place()
    greet([partner])()
    total = both_parts(part_ref, rcv, partner, e_send, e_recv)
    vel = kick(vel_ref[...], pos_ref[...], total, rate)
    vel_new[...] = vel
    pos_new[...] = pos_ref[...] + step_size * vel


def finish(rate, hidden, part_ref, pos_ref, vel_ref, all_ref, rcv, e_send, e_recv, o_send, o_recv, s_send, s_recv):
    core, _, coords, partner, device_at = place()
    greet(torus_neighbours(coords, device_at) + [partner])()
    total = both_parts(part_ref, rcv, partner, e_send, e_recv)
    lane, sub = grids()
    pos = pos_ref[...]
    vel = kick(vel_ref[...], pos, total, rate)
    loss = total[:1, LOSS:LOSS + 1]
    square = (pos * pos) * (1.0 / (2.0 * PRIOR_VAR)) + 0.5 * (vel * vel)
    energy = loss + jnp.sum(jnp.sum(square, axis=1, keepdims=True), axis=0, keepdims=True)
    tails = []
    for value in (pos, vel):
        w2 = jnp.broadcast_to(value[:, OUT:OUT + 1], (HID, LANES))
        row = jnp.concatenate([w2, jnp.zeros((LANES - HID, LANES), jnp.float32)], axis=0).T[:1, :]
        tails.append(jnp.broadcast_to(row, (HID, LANES)))
    tails[0] = jnp.where(lane == hidden, energy, tails[0])
    outs = [jnp.where(sub == hidden, t, v) for t, v in zip(tails, (pos, vel))]
    all_ref[core, coords[0], coords[1], coords[2]] = jnp.where(core == 0, outs[0], outs[1])
    o_descs = torus_gather(all_ref.at[core], OUT_PIECES, coords, device_at, o_send, o_recv)
    swap = pltpu.make_async_remote_copy(
        src_ref=all_ref.at[core], dst_ref=all_ref.at[core], send_sem=s_send, recv_sem=s_recv,
        device_id={'data': partner}, device_id_type=pl.DeviceIdType.MESH)
    swap.start()
    for d in o_descs:
        d.wait_send()
    swap.wait_send()
    pltpu.make_async_remote_copy(
        src_ref=all_ref.at[1 - core], dst_ref=all_ref.at[1 - core], send_sem=s_send, recv_sem=s_recv,
        device_id={'data': partner}, device_id_type=pl.DeviceIdType.MESH).wait_recv()


def spread_out(flat, w_end, wo_end, m_end, mo_end, e_end):
    hidden, _, num_feat = w_end.shape

    def spread(h, carry):
        for n, ref in enumerate((w_end, m_end)):
            for c in range(0, BLOCKS, 8):
                ref[h, c:c + 8, :] = flat[n, pl.ds(c * HID + h, 8, stride=HID), :][:, :num_feat]
        return carry

    lax.fori_loop(0, hidden, spread, 0)
    for n, ref in enumerate((wo_end, mo_end)):
        tail = jnp.concatenate([flat[n, pl.ds(c * HID + hidden, 8, stride=HID), :] for c in range(0, BLOCKS, 8)]
                               + [jnp.zeros((LANES - BLOCKS, LANES), jnp.float32)], axis=0).T
        ref[...] = tail[:hidden, :BLOCKS]
        if n == 0:
            e_end[...] = tail[hidden:hidden + 1, :BLOCKS]


VMEM = pl.BlockSpec(memory_space=pltpu.VMEM)
HBM = pl.BlockSpec(memory_space=pltpu.HBM)
DMA = pltpu.SemaphoreType.DMA


def struct(shape, dtype=jnp.float32):
    return jax.ShapeDtypeStruct(shape, dtype)


def call(kernel, name, inputs, outs, scratch, mib, collective=None, in_specs=None):
    extra = {} if collective is None else dict(collective_id=collective, has_side_effects=True)
    return pl.pallas_call(
        kernel, out_shape=outs, in_specs=in_specs or [VMEM] * len(inputs),
        out_specs=[VMEM] * len(outs) if isinstance(outs, list) else VMEM, scratch_shapes=scratch,
        compiler_params=pltpu.CompilerParams(vmem_limit_bytes=mib * MIB, **extra), name=name)(*inputs)


def grad_call(data, pos, with_loss):
    bf16 = jnp.bfloat16
    return call(functools.partial(gradient, with_loss), 'gradient', (*data, pos), struct((HID, LANES)), [
        pltpu.VMEM((BLOCKS, 8, LANES), jnp.float32),
        pltpu.VMEM((HID, LANES), jnp.float32),
        pltpu.VMEM((2, 2 * HID, LANES), bf16),
        pltpu.VMEM((2, 4, 2 * HID, LANES), bf16)], 4)


def run_all(feats, labels, w_in, w_out, mom_in, mom_out, step_size):
    rows, num_feat = feats.shape
    hidden, chains, _ = w_in.shape
    f32, bf16 = jnp.float32, jnp.bfloat16
    state = struct((HID, LANES))
    outs = [struct((SIDE, SIDE, SIDE, rows, LANES), bf16), struct((BLOCKS, rows // LANES, LANES, LANES), bf16), struct((BLOCKS, 8, LANES)), state, state]
    *data, pos, vel = call(
        collect_rows, 'collect', (feats, labels, w_in, w_out, mom_in, mom_out), outs,
        [pltpu.VMEM((rows, num_feat), bf16), pltpu.VMEM((2, hidden, 8, num_feat), f32), DMA((3, 36)), DMA((3, 36)), DMA((3,))],
        4, 0, [HBM, VMEM, HBM, VMEM, HBM, VMEM])
    for k in range(LEAPS):
        part = grad_call(data, pos, False)
        rate = 0.5 * step_size if k == 0 else step_size
        pos, vel = call(functools.partial(leap, rate, step_size), 'leap', (part, pos, vel), [state, state],
                        [pltpu.VMEM((HID, LANES), f32), DMA, DMA], 1, 1 if k == 0 else 2)
    part = grad_call(data, pos, True)
    every = call(functools.partial(finish, 0.5 * step_size, hidden), 'finish', (part, pos, vel), struct((2, SIDE, SIDE, SIDE, HID, LANES)),
                 [pltpu.VMEM((HID, LANES), f32), DMA, DMA, DMA((3, 36)), DMA((3, 36)), DMA, DMA], 2, 3)
    ends = [struct(w_in.shape), struct(w_out.shape)] * 2 + [struct((1, chains))]
    return call(spread_out, 'spread', (every.reshape(2, BLOCKS * HID, LANES),), ends, [], 8)


def solution(mesh):
    row_spec = P('data', None)
    label_spec = P('data')
    in_spec = P(None, 'parts', None)
    out_spec = P('parts', None)
    chain_spec = P('parts')

    def run_chains(feats, labels, w_in, w_out, mom_in, mom_out):
        num_rows, num_feat = feats.shape
        hidden = w_in.shape[2]
        step_size = 1.0 / math.sqrt(num_rows * (num_feat + hidden))

        def device_body(x_rows, y_rows, pos_in, pos_out, vel_in, vel_out):
            turned = [jnp.transpose(v) for v in (pos_in, pos_out, vel_in, vel_out)]
            ends = run_all(x_rows, y_rows.reshape(8, LANES), *turned, step_size)
            return tuple(jnp.transpose(v) for v in ends[:4]) + (ends[4].reshape(-1),)

        mapped = jax.shard_map(device_body, mesh=mesh, in_specs=(row_spec, label_spec, in_spec, out_spec, in_spec, out_spec), out_specs=(in_spec, out_spec, in_spec, out_spec, chain_spec), check_vma=False)
        return mapped(feats, labels, w_in, w_out, mom_in, mom_out)

    return run_chains
```

```python
import functools
import math

import jax
import jax.numpy as jnp
from jax import lax
from jax.experimental import pallas as pl
from jax.experimental.pallas import tpu as pltpu
from jax.sharding import PartitionSpec as P

LEAPS = 16
PRIOR_VAR = 1.0
SIDE = 4
BLOCKS = SIDE ** 3
HID = 56
LANES = 128
LAB = 123
LOSS = 124
OUT = 127
UNROLL = 8
MIB = 2 ** 20
PREPARE_BYTES = 57000000
ROW_PIECES = ((0, 344, 176), (344, 344, 176), (688, 336, 168))
OUT_PIECES = ((0, 24, 16), (24, 16, 8), (40, 16, 8))


def torus_gather(buf, pieces, coords, device_at, send_sem, recv_sem, near=None, middle=None, share=None):
    descs = []
    direct = share is not None
    plus = lambda c, d: lax.rem(c + d + SIDE, SIDE)

    def view(p, where, part):
        start, size, first = pieces[p]
        lo, n = {0: (start, size), 1: (start, first), 2: (start + first, size - first)}[part]
        return buf.at[where[0], where[1], where[2], pl.ds(lo, n), :]

    def copy(p, where, part, axis, step, slot):
        to = list(coords)
        to[axis] = plus(to[axis], step)
        ref = view(p, where, part)
        return pltpu.make_async_remote_copy(
            src_ref=ref, dst_ref=ref, send_sem=send_sem.at[p, slot], recv_sem=recv_sem.at[p, slot],
            device_id={'data': device_at(to)}, device_id_type=pl.DeviceIdType.MESH)

    def send(p, where, part, axis, step, slot):
        c = copy(p, where, part, axis, step, slot)
        c.start()
        descs.append(c)

    def wait(p, where, part, axis, step, slot):
        copy(p, where, part, axis, step, slot).wait_recv()

    orders = [(p, (p + 1) % 3, (p + 2) % 3) for p in range(3)]
    OFFS = (0, -1, 1, 2)

    def at(p, off0, off1, off2):
        where = [None, None, None]
        for axis, off in zip(orders[p], (off0, off1, off2)):
            where[axis] = slice(None) if off is None else (coords[axis] if off == 0 else plus(coords[axis], off))
        return where

    def start_full(p, ph, own, base):
        axis = orders[p][ph]
        send(p, own, 0, axis, 1, base)
        send(p, own, 0, axis, -1, base + 1)
        if direct and ph < 2:
            send(p, own, 0, axis, 2, base + 2)

    def relay(p, ph, low, high, base):
        axis = orders[p][ph]
        wait(p, low, 0, axis, 1, base)
        if direct and ph < 2:
            wait(p, high, 0, axis, 1, base + 1)
            return
        send(p, low, 1, axis, 1, base + 2)
        wait(p, high, 0, axis, 1, base + 1)
        send(p, high, 2, axis, -1, base + 3)

    def finish(p, ph, far, base):
        axis = orders[p][ph]
        if direct and ph < 2:
            wait(p, far, 0, axis, 1, base + 2)
            return
        wait(p, far, 1, axis, 1, base + 2)
        wait(p, far, 2, axis, 1, base + 3)

    B1, B2, B3 = 0, 4, 20
    for p in range(3):
        start_full(p, 0, at(p, 0, 0, 0), B1)
    for p in range(3):
        start_full(p, 1, at(p, 0, 0, 0), B2)
    for p in range(3):
        relay(p, 0, at(p, -1, 0, 0), at(p, 1, 0, 0), B1)
        start_full(p, 1, at(p, -1, 0, 0), B2 + 4)
        start_full(p, 1, at(p, 1, 0, 0), B2 + 8)
    for p in range(3):
        finish(p, 0, at(p, 2, 0, 0), B1)
        start_full(p, 1, at(p, 2, 0, 0), B2 + 12)
        start_full(p, 2, at(p, None, 0, 0), B3)
    for q in range(4):
        for p in range(3):
            relay(p, 1, at(p, OFFS[q], -1, 0), at(p, OFFS[q], 1, 0), B2 + 4 * q)
    for p in range(3):
        start_full(p, 2, at(p, None, -1, 0), B3 + 4)
        start_full(p, 2, at(p, None, 1, 0), B3 + 8)
    for q in range(4):
        for p in range(3):
            finish(p, 1, at(p, OFFS[q], 2, 0), B2 + 4 * q)
    for p in range(3):
        start_full(p, 2, at(p, None, 2, 0), B3 + 12)
    for q in range(4):
        for p in range(3):
            relay(p, 2, at(p, None, OFFS[q], -1), at(p, None, OFFS[q], 1), B3 + 4 * q)
    if near is not None:
        near()
    if share is not None:
        for p in range(3):
            for i in range(3):
                share(p, i, at(p, None, None, OFFS[i]))
    for q in range(4):
        if q == 3 and middle is not None:
            middle()
        for p in range(3):
            finish(p, 2, at(p, None, OFFS[q], 2), B3 + 4 * q)
    if share is not None:
        for p in range(3):
            share(p, 3, at(p, None, None, 2))
    return descs


def block_index(b):
    return b // (SIDE * SIDE), (b // SIDE) % SIDE, b % SIDE


def place():
    me = lax.axis_index('data')
    core = me % 2
    chip = me // 2
    coords = (chip // (SIDE * SIDE), (chip // SIDE) % SIDE, chip % SIDE)

    def device_at(c):
        return ((c[0] * SIDE + c[1]) * SIDE + c[2]) * 2 + core

    return core, chip, coords, me + 1 - 2 * core, device_at


def greet(devices):
    barrier = pltpu.get_barrier_semaphore()
    for device in devices:
        pl.semaphore_signal(barrier, inc=1, device_id={'data': device}, device_id_type=pl.DeviceIdType.MESH)
    return lambda: pl.semaphore_wait(barrier, len(devices))


def torus_neighbours(coords, device_at, steps=(1, -1)):
    found = []
    for axis in range(3):
        for step in steps:
            to = list(coords)
            to[axis] = lax.rem(to[axis] + step + SIDE, SIDE)
            found.append(device_at(to))
    return found


def grids():
    lane = lax.broadcasted_iota(jnp.int32, (HID, LANES), 1)
    sub = lax.broadcasted_iota(jnp.int32, (HID, LANES), 0)
    return lane, sub


def prepare(feat_ref, lab_ref, w_ref, wo_ref, m_ref, mo_ref, own_ref, pos_ref, vel_ref, x_in, w_tmp, lab_tmp, o_tmp, sem):
    num_feat = feat_ref.shape[1]
    hidden = w_ref.shape[0]
    chip = lax.axis_index('data') // 2
    eight = pl.multiple_of((chip // 8) * 8, 8)
    loads = [pltpu.make_async_copy(feat_ref, x_in, sem.at[0]), pltpu.make_async_copy(lab_ref, lab_tmp, sem.at[1])]
    for n, ref in enumerate((w_ref, m_ref)):
        loads.append(pltpu.make_async_copy(ref.at[:, pl.ds(eight, 8), :], w_tmp.at[n], sem.at[n + 2]))
    for n, ref in enumerate((wo_ref, mo_ref)):
        loads.append(pltpu.make_async_copy(ref, o_tmp.at[n], sem.at[n + 4]))
    for load in loads:
        load.start()
    pos_ref[...] = jnp.zeros_like(pos_ref)
    vel_ref[...] = jnp.zeros_like(vel_ref)
    for load in loads:
        load.wait()
    labels = lab_tmp[...].astype(jnp.float32)
    for k in range(8):
        column = jnp.broadcast_to(labels[k:k + 1, :], (LANES, LANES)).T
        spare = lax.broadcasted_iota(jnp.int32, (LANES, LANES), 1)
        rows = pl.ds(k * LANES, LANES)
        own_ref[rows, :] = jnp.where(spare == LAB, column, 0.0).astype(jnp.bfloat16)
        own_ref[rows, :num_feat] = x_in[rows, :]
    chain_row = lax.broadcasted_iota(jnp.int32, (hidden, 8, num_feat), 1) == chip % 8
    chain_lane = lax.broadcasted_iota(jnp.int32, wo_ref.shape, 1) == chip
    for n, ref in enumerate((pos_ref, vel_ref)):
        ref[:hidden, :num_feat] = jnp.sum(jnp.where(chain_row, w_tmp[n], 0.0), axis=1)
        ref[:hidden, OUT:OUT + 1] = jnp.sum(jnp.where(chain_lane, o_tmp[n], 0.0), axis=1, keepdims=True)


def collect_rows(own_ref, x_all, xt_all, y_all, x_send, x_recv, own_sem):
    core, chip, coords, partner, device_at = place()
    own = pltpu.make_async_copy(own_ref, x_all.at[coords[0], coords[1], coords[2]], own_sem)
    own.start()
    ready = greet(torus_neighbours(coords, device_at))
    own.wait()
    ready()

    def turn(where):
        z, y, x = where
        b = (z * SIDE + y) * SIDE + x
        for k in range(8):
            xt = x_all[z, y, x, k * LANES:(k + 1) * LANES, :].T
            xt_all[b, k] = xt
            y_all[b, k:k + 1, :] = xt[112:128, :].astype(jnp.float32)[LAB - 112:LAB - 111, :]

    def moved(offsets):
        return tuple(lax.rem(c + o, SIDE) for c, o in zip(coords, offsets))

    def three(i):
        return 3 + i

    def near():
        def body(i, carry):
            turn(moved((three(i // 9), three((i // 3) % 3), three(i % 3))))
            return carry
        lax.fori_loop(0, 27, body, 0)

    def middle():
        def body(i, carry):
            u, v = three(i // 3), three(i % 3)
            turn(moved((2, u, v)))
            turn(moved((u, 2, v)))
            turn(moved((u, v, 2)))
            return carry
        lax.fori_loop(0, 9, body, 0)

    def far():
        def body(i, carry):
            u = three(i)
            turn(moved((2, 2, u)))
            turn(moved((2, u, 2)))
            turn(moved((u, 2, 2)))
            return carry
        lax.fori_loop(0, 3, body, 0)
        turn(moved((2, 2, 2)))

    x_descs = torus_gather(x_all, ROW_PIECES, coords, device_at, x_send, x_recv, near, middle)
    far()
    for d in x_descs:
        d.wait_send()


def gradient(with_loss, *refs):
    def with_acc(pre, grad):
        gradient_body(with_loss, pre, grad, *refs)

    def spec(q):
        return pltpu.ACC(q)((2 * HID, 2 * LANES), jnp.float32)

    pl.run_scoped(with_acc, ((spec(0), spec(1)), (spec(0), spec(1))), (spec(0), spec(1)))


def gradient_body(with_loss, pre_acc, grad_acc, x_all, xt_all, y_all, pos_ref, part_ref, z_all, w2_ref, wbd_ref, b_ref):
    lane, sub = grids()
    def push_forward(b):
        for q in range(2):
            tiles = [jnp.concatenate([xt_all[b, 4 * s + 2 * q], xt_all[b, 4 * s + 2 * q + 1]], axis=1) for s in range(2)]
            pltpu.matmul_push_rhs(jnp.concatenate(tiles, axis=0), staging_register=0, mxu_index=q)

    def forward(u):
        wbd = jnp.concatenate([wbd_ref[0], wbd_ref[1]], axis=1)
        for q in range(2):
            pltpu.matmul_acc_lhs(pre_acc[u][q], wbd, load_staged_rhs=0)

    def rows_to_back(b, u, acc):
        w2 = w2_ref[...].reshape(HID // 8, 8, LANES)
        for q in range(2):
            act = jnp.tanh(pltpu.matmul_pop(pre_acc[u][q]))
            for h in range(2):
                j = 2 * q + h
                parts = []
                for s in range(2):
                    k = 4 * s + j
                    part = act[s * HID:(s + 1) * HID, h * LANES:(h + 1) * LANES].reshape(HID // 8, 8, LANES)
                    z = jnp.sum(part * w2, axis=0)
                    for shift in (4, 2, 1):
                        z = z + pltpu.roll(z, shift, 0)
                    if with_loss:
                        z_all[b, k:k + 1, :] = z[:1]
                    res = jnp.broadcast_to(y_all[b, k:k + 1, :], (8, LANES)) - 1.0 / (1.0 + jnp.exp(-z))
                    weighed = part * res
                    acc = acc + weighed
                    parts.append(((res - weighed * part) * w2).reshape(HID, LANES))
                b_ref[u, j] = jnp.concatenate(parts, axis=0).astype(jnp.bfloat16)
        return acc

    def push_grad(b):
        z, y, x = block_index(b)
        rows = x_all.at[z, y, x]
        for q in range(2):
            tile = jnp.concatenate([rows[256 * q:256 * q + 256, :], rows[512 + 256 * q:768 + 256 * q, :]], axis=1)
            pltpu.matmul_push_rhs(tile, staging_register=1, mxu_index=q)

    def weight_grad(u):
        for q in range(2):
            lhs = jnp.concatenate([b_ref[u, 2 * q], b_ref[u, 2 * q + 1]], axis=1)
            pltpu.matmul_acc_lhs(grad_acc[q], lhs, load_staged_rhs=1)

    pos = pos_ref[...]
    w_in = jnp.where(lane < LAB, pos, 0.0)
    nil = jnp.zeros_like(w_in)
    wbd_ref[0] = jnp.concatenate([w_in, nil], axis=0).astype(jnp.bfloat16)
    wbd_ref[1] = jnp.concatenate([nil, w_in], axis=0).astype(jnp.bfloat16)
    w2_ref[...] = jnp.broadcast_to(pos[:, OUT:OUT + 1], (HID, LANES))
    b_ref[1] = jnp.zeros((4, 2 * HID, LANES), jnp.bfloat16)
    for u in range(2):
        push_forward(u)
        forward(u)
    push_forward(2)
    push_grad(0)

    def pair(i, acc):
        for v in range(UNROLL):
            u = v % 2
            n = UNROLL * i + v
            acc = rows_to_back(n, u, acc)
            forward(u)
            push_forward(jnp.minimum(n + 3, BLOCKS - 1))
            weight_grad(1 - u)
            push_grad(n)
        return acc

    acc = lax.fori_loop(0, BLOCKS // UNROLL, pair, jnp.zeros((HID // 8, 8, LANES), jnp.float32)).reshape(HID, LANES)
    weight_grad(1)
    for u in range(2):
        if u == 0:
            forward(u)
        for q in range(2):
            pltpu.matmul_pop(pre_acc[u][q])
    whole = pltpu.matmul_pop(grad_acc[0]) + pltpu.matmul_pop(grad_acc[1])
    grad = whole[:HID, :LANES] + whole[HID:, LANES:]
    grad = jnp.where(lane < LAB, grad, jnp.where(lane == OUT, jnp.sum(acc, axis=1, keepdims=True), 0.0))
    if with_loss:
        def loss_block(b, total):
            z = z_all[b]
            return total + (jnp.maximum(z, 0.0) + jnp.log1p(jnp.exp(-jnp.abs(z))) - y_all[b] * z)

        total = lax.fori_loop(0, BLOCKS, loss_block, jnp.zeros((8, LANES), jnp.float32))
        total = jnp.sum(jnp.sum(total, axis=1, keepdims=True), axis=0, keepdims=True)
        grad = jnp.where((lane == LOSS) & (sub == 0), total, grad)
    part_ref[...] = grad


def both_parts(part_ref, rcv, partner, e_send, e_recv):
    ex = pltpu.make_async_remote_copy(
        src_ref=part_ref, dst_ref=rcv, send_sem=e_send, recv_sem=e_recv,
        device_id={'data': partner}, device_id_type=pl.DeviceIdType.MESH)
    ex.start()
    ex.wait()
    return part_ref[...] + rcv[...]


def kick(vel, pos, total, rate):
    lane, _ = grids()
    is_param = (lane < LAB) | (lane == OUT)
    return vel + rate * jnp.where(is_param, total - pos * (1.0 / PRIOR_VAR), 0.0)


def leap(rate, step_size, part_ref, pos_ref, vel_ref, pos_new, vel_new, rcv, e_send, e_recv):
    _, _, _, partner, _ = place()
    greet([partner])()
    total = both_parts(part_ref, rcv, partner, e_send, e_recv)
    vel = kick(vel_ref[...], pos_ref[...], total, rate)
    vel_new[...] = vel
    pos_new[...] = pos_ref[...] + step_size * vel


def finish(rate, hidden, part_ref, pos_ref, vel_ref, all_ref, rcv, e_send, e_recv, o_send, o_recv, s_send, s_recv):
    core, _, coords, partner, device_at = place()
    greet(torus_neighbours(coords, device_at, (1, -1, 2)) + [partner])()
    total = both_parts(part_ref, rcv, partner, e_send, e_recv)
    lane, sub = grids()
    pos = pos_ref[...]
    vel = kick(vel_ref[...], pos, total, rate)
    loss = total[:1, LOSS:LOSS + 1]
    square = (pos * pos) * (1.0 / (2.0 * PRIOR_VAR)) + 0.5 * (vel * vel)
    energy = loss + jnp.sum(jnp.sum(square, axis=1, keepdims=True), axis=0, keepdims=True)
    tails = []
    for value in (pos, vel):
        w2 = jnp.broadcast_to(value[:, OUT:OUT + 1], (HID, LANES))
        row = jnp.concatenate([w2, jnp.zeros((LANES - HID, LANES), jnp.float32)], axis=0).T[:1, :]
        tails.append(jnp.broadcast_to(row, (HID, LANES)))
    tails[0] = jnp.where(lane == hidden, energy, tails[0])
    outs = [jnp.where(sub == hidden, t, v) for t, v in zip(tails, (pos, vel))]
    all_ref[core, coords[0], coords[1], coords[2]] = jnp.where(core == 0, outs[0], outs[1])
    shared = []

    def across(side, p, i, where):
        start, size, _ = OUT_PIECES[p]
        ref = all_ref.at[side, where[0], where[1], where[2], pl.ds(start, size), :]
        return pltpu.make_async_remote_copy(
            src_ref=ref, dst_ref=ref, send_sem=s_send.at[p, i], recv_sem=s_recv.at[p, i],
            device_id={'data': partner}, device_id_type=pl.DeviceIdType.MESH)

    def share(p, i, where):
        across(core, p, i, where).start()
        shared.append((p, i, where))

    o_descs = torus_gather(all_ref.at[core], OUT_PIECES, coords, device_at, o_send, o_recv, share=share)
    for d in o_descs:
        d.wait_send()
    for item in shared:
        across(core, *item).wait_send()
        across(1 - core, *item).wait_recv()


def spread_out(flat, w_end, wo_end, m_end, mo_end, e_end):
    hidden, _, num_feat = w_end.shape

    def spread(h, carry):
        for n, ref in enumerate((w_end, m_end)):
            for c in range(0, BLOCKS, 8):
                ref[h, c:c + 8, :] = flat[n, pl.ds(c * HID + h, 8, stride=HID), :][:, :num_feat]
        return carry

    lax.fori_loop(0, hidden, spread, 0)
    for n, ref in enumerate((wo_end, mo_end)):
        tail = jnp.concatenate([flat[n, pl.ds(c * HID + hidden, 8, stride=HID), :] for c in range(0, BLOCKS, 8)]
                               + [jnp.zeros((LANES - BLOCKS, LANES), jnp.float32)], axis=0).T
        ref[...] = tail[:hidden, :BLOCKS]
        if n == 0:
            e_end[...] = tail[hidden:hidden + 1, :BLOCKS]


VMEM = pl.BlockSpec(memory_space=pltpu.VMEM)
HBM = pl.BlockSpec(memory_space=pltpu.HBM)
DMA = pltpu.SemaphoreType.DMA


def struct(shape, dtype=jnp.float32):
    return jax.ShapeDtypeStruct(shape, dtype)


def call(kernel, name, inputs, outs, scratch, limit, collective=None, in_specs=None):
    extra = {} if collective is None else dict(collective_id=collective, has_side_effects=True)
    return pl.pallas_call(
        kernel, out_shape=outs, in_specs=in_specs or [VMEM] * len(inputs),
        out_specs=[VMEM] * len(outs) if isinstance(outs, list) else VMEM, scratch_shapes=scratch,
        compiler_params=pltpu.CompilerParams(vmem_limit_bytes=limit, **extra), name=name)(*inputs)


def grad_call(data, pos, with_loss):
    bf16 = jnp.bfloat16
    return call(functools.partial(gradient, with_loss), 'gradient', (*data, pos), struct((HID, LANES)), [
        pltpu.VMEM((BLOCKS, 8, LANES), jnp.float32),
        pltpu.VMEM((HID, LANES), jnp.float32),
        pltpu.VMEM((2, 2 * HID, LANES), bf16),
        pltpu.VMEM((2, 4, 2 * HID, LANES), bf16)], 4 * MIB)


def run_all(feats, labels, w_in, w_out, mom_in, mom_out, step_size):
    rows, num_feat = feats.shape
    hidden, chains, _ = w_in.shape
    f32, bf16 = jnp.float32, jnp.bfloat16
    state = struct((HID, LANES))
    own, pos, vel = call(
        prepare, 'prepare', (feats, labels, w_in, w_out, mom_in, mom_out), [struct((rows, LANES), bf16), state, state],
        [pltpu.VMEM((rows, num_feat), bf16), pltpu.VMEM((2, hidden, 8, num_feat), f32), pltpu.VMEM((8, LANES), jnp.int32), pltpu.VMEM((2, hidden, chains), f32), DMA((6,))],
        PREPARE_BYTES, None, [HBM] * 6)
    outs = [struct((SIDE, SIDE, SIDE, rows, LANES), bf16), struct((BLOCKS, rows // LANES, LANES, LANES), bf16), struct((BLOCKS, 8, LANES))]
    data = call(collect_rows, 'collect', (own,), outs, [DMA((3, 36)), DMA((3, 36)), DMA], 2 * MIB, 0)
    for k in range(LEAPS):
        part = grad_call(data, pos, False)
        rate = 0.5 * step_size if k == 0 else step_size
        pos, vel = call(functools.partial(leap, rate, step_size), 'leap', (part, pos, vel), [state, state],
                        [pltpu.VMEM((HID, LANES), f32), DMA, DMA], MIB, 1 if k == 0 else 2)
    part = grad_call(data, pos, True)
    every = call(functools.partial(finish, 0.5 * step_size, hidden), 'finish', (part, pos, vel), struct((2, SIDE, SIDE, SIDE, HID, LANES)),
                 [pltpu.VMEM((HID, LANES), f32), DMA, DMA, DMA((3, 36)), DMA((3, 36)), DMA((3, 4)), DMA((3, 4))], 2 * MIB, 3)
    ends = [struct(w_in.shape), struct(w_out.shape)] * 2 + [struct((1, chains))]
    return call(spread_out, 'spread', (every.reshape(2, BLOCKS * HID, LANES),), ends, [], 8 * MIB)


def solution(mesh):
    row_spec = P('data', None)
    label_spec = P('data')
    in_spec = P(None, 'parts', None)
    out_spec = P('parts', None)
    chain_spec = P('parts')

    def run_chains(feats, labels, w_in, w_out, mom_in, mom_out):
        num_rows, num_feat = feats.shape
        hidden = w_in.shape[2]
        step_size = 1.0 / math.sqrt(num_rows * (num_feat + hidden))

        def device_body(x_rows, y_rows, pos_in, pos_out, vel_in, vel_out):
            turned = [jnp.transpose(v) for v in (pos_in, pos_out, vel_in, vel_out)]
            ends = run_all(x_rows, y_rows.reshape(8, LANES), *turned, step_size)
            return tuple(jnp.transpose(v) for v in ends[:4]) + (ends[4].reshape(-1),)

        mapped = jax.shard_map(device_body, mesh=mesh, in_specs=(row_spec, label_spec, in_spec, out_spec, in_spec, out_spec), out_specs=(in_spec, out_spec, in_spec, out_spec, chain_spec), check_vma=False)
        return mapped(feats, labels, w_in, w_out, mom_in, mom_out)

    return run_chains
```

```python
import functools
import math

import jax
import jax.numpy as jnp
from jax import lax
from jax.experimental import pallas as pl
from jax.experimental.pallas import tpu as pltpu
from jax.sharding import PartitionSpec as P

LEAPS = 16
PRIOR_VAR = 1.0
SIDE = 4
BLOCKS = SIDE ** 3
HID = 56
LANES = 128
LAB = 123
LOSS = 124
OUT = 127
UNROLL = 8
MIB = 2 ** 20
PREPARE_BYTES = 57000000
ROW_PIECES = ((0, 344, 176), (344, 344, 176), (688, 336, 168))
OUT_PIECES = ((0, 24, 16), (24, 16, 8), (40, 16, 8))


def torus_gather(buf, pieces, coords, device_at, send_sem, recv_sem, near=None, middle=None, share=None):
    descs = []
    direct = share is not None
    plus = lambda c, d: lax.rem(c + d + SIDE, SIDE)

    def view(p, where, part):
        start, size, first = pieces[p]
        lo, n = {0: (start, size), 1: (start, first), 2: (start + first, size - first)}[part]
        return buf.at[where[0], where[1], where[2], pl.ds(lo, n), :]

    def copy(p, where, part, axis, step, slot):
        to = list(coords)
        to[axis] = plus(to[axis], step)
        ref = view(p, where, part)
        return pltpu.make_async_remote_copy(
            src_ref=ref, dst_ref=ref, send_sem=send_sem.at[p, slot], recv_sem=recv_sem.at[p, slot],
            device_id={'data': device_at(to)}, device_id_type=pl.DeviceIdType.MESH)

    def send(p, where, part, axis, step, slot):
        c = copy(p, where, part, axis, step, slot)
        c.start()
        descs.append(c)

    def wait(p, where, part, axis, step, slot):
        copy(p, where, part, axis, step, slot).wait_recv()

    orders = [(p, (p + 1) % 3, (p + 2) % 3) for p in range(3)]
    OFFS = (0, -1, 1, 2)

    def at(p, off0, off1, off2):
        where = [None, None, None]
        for axis, off in zip(orders[p], (off0, off1, off2)):
            where[axis] = slice(None) if off is None else (coords[axis] if off == 0 else plus(coords[axis], off))
        return where

    def start_full(p, ph, own, base):
        axis = orders[p][ph]
        send(p, own, 0, axis, 1, base)
        send(p, own, 0, axis, -1, base + 1)
        if direct and ph < 2:
            send(p, own, 0, axis, 2, base + 2)

    def relay(p, ph, low, high, base):
        axis = orders[p][ph]
        wait(p, low, 0, axis, 1, base)
        if direct and ph < 2:
            wait(p, high, 0, axis, 1, base + 1)
            return
        send(p, low, 1, axis, 1, base + 2)
        wait(p, high, 0, axis, 1, base + 1)
        send(p, high, 2, axis, -1, base + 3)

    def finish(p, ph, far, base):
        axis = orders[p][ph]
        if direct and ph < 2:
            wait(p, far, 0, axis, 1, base + 2)
            return
        wait(p, far, 1, axis, 1, base + 2)
        wait(p, far, 2, axis, 1, base + 3)

    B1, B2, B3 = 0, 4, 20
    for p in range(3):
        start_full(p, 0, at(p, 0, 0, 0), B1)
    for p in range(3):
        start_full(p, 1, at(p, 0, 0, 0), B2)
    for p in range(3):
        relay(p, 0, at(p, -1, 0, 0), at(p, 1, 0, 0), B1)
        start_full(p, 1, at(p, -1, 0, 0), B2 + 4)
        start_full(p, 1, at(p, 1, 0, 0), B2 + 8)
    for p in range(3):
        finish(p, 0, at(p, 2, 0, 0), B1)
        start_full(p, 1, at(p, 2, 0, 0), B2 + 12)
        start_full(p, 2, at(p, None, 0, 0), B3)
    for q in range(4):
        for p in range(3):
            relay(p, 1, at(p, OFFS[q], -1, 0), at(p, OFFS[q], 1, 0), B2 + 4 * q)
    for p in range(3):
        start_full(p, 2, at(p, None, -1, 0), B3 + 4)
        start_full(p, 2, at(p, None, 1, 0), B3 + 8)
    for q in range(4):
        for p in range(3):
            finish(p, 1, at(p, OFFS[q], 2, 0), B2 + 4 * q)
    for p in range(3):
        start_full(p, 2, at(p, None, 2, 0), B3 + 12)
    for q in range(4):
        if q == 3 and near is not None:
            near()
        for p in range(3):
            relay(p, 2, at(p, None, OFFS[q], -1), at(p, None, OFFS[q], 1), B3 + 4 * q)
    if share is not None:
        for p in range(3):
            for i in range(3):
                share(p, i, at(p, None, None, OFFS[i]))
    for q in range(4):
        if q == 3 and middle is not None:
            middle()
        for p in range(3):
            finish(p, 2, at(p, None, OFFS[q], 2), B3 + 4 * q)
    if share is not None:
        for p in range(3):
            share(p, 3, at(p, None, None, 2))
    return descs


def block_index(b):
    return b // (SIDE * SIDE), (b // SIDE) % SIDE, b % SIDE


def place():
    me = lax.axis_index('data')
    core = me % 2
    chip = me // 2
    coords = (chip // (SIDE * SIDE), (chip // SIDE) % SIDE, chip % SIDE)

    def device_at(c):
        return ((c[0] * SIDE + c[1]) * SIDE + c[2]) * 2 + core

    return core, chip, coords, me + 1 - 2 * core, device_at


def greet(devices):
    barrier = pltpu.get_barrier_semaphore()
    for device in devices:
        pl.semaphore_signal(barrier, inc=1, device_id={'data': device}, device_id_type=pl.DeviceIdType.MESH)
    return lambda: pl.semaphore_wait(barrier, len(devices))


def torus_neighbours(coords, device_at, steps=(1, -1)):
    found = []
    for axis in range(3):
        for step in steps:
            to = list(coords)
            to[axis] = lax.rem(to[axis] + step + SIDE, SIDE)
            found.append(device_at(to))
    return found


def grids():
    lane = lax.broadcasted_iota(jnp.int32, (HID, LANES), 1)
    sub = lax.broadcasted_iota(jnp.int32, (HID, LANES), 0)
    return lane, sub


def set_weights(pos, wbd_ref, w2_ref):
    lane, _ = grids()
    w_in = jnp.where(lane < LAB, pos, 0.0)
    nil = jnp.zeros_like(w_in)
    wbd_ref[0] = jnp.concatenate([w_in, nil], axis=0).astype(jnp.bfloat16)
    wbd_ref[1] = jnp.concatenate([nil, w_in], axis=0).astype(jnp.bfloat16)
    w2_ref[...] = jnp.broadcast_to(pos[:, OUT:OUT + 1], (HID, LANES))


def whole_gradient(whole, acc):
    lane, _ = grids()
    grad = whole[:HID, :LANES] + whole[HID:, LANES:]
    return jnp.where(lane < LAB, grad, jnp.where(lane == OUT, jnp.sum(acc, axis=1, keepdims=True), 0.0))


def prepare(feat_ref, lab_ref, w_ref, wo_ref, m_ref, mo_ref, own_ref, pos_ref, vel_ref, x_in, w_tmp, lab_tmp, o_tmp, sem):
    num_feat = feat_ref.shape[1]
    hidden = w_ref.shape[0]
    chip = lax.axis_index('data') // 2
    eight = pl.multiple_of((chip // 8) * 8, 8)
    loads = [pltpu.make_async_copy(feat_ref, x_in, sem.at[0]), pltpu.make_async_copy(lab_ref, lab_tmp, sem.at[1])]
    for n, ref in enumerate((w_ref, m_ref)):
        loads.append(pltpu.make_async_copy(ref.at[:, pl.ds(eight, 8), :], w_tmp.at[n], sem.at[n + 2]))
    for n, ref in enumerate((wo_ref, mo_ref)):
        loads.append(pltpu.make_async_copy(ref, o_tmp.at[n], sem.at[n + 4]))
    for load in loads:
        load.start()
    pos_ref[...] = jnp.zeros_like(pos_ref)
    vel_ref[...] = jnp.zeros_like(vel_ref)
    for load in loads:
        load.wait()
    labels = lab_tmp[...].astype(jnp.float32)
    for k in range(8):
        column = jnp.broadcast_to(labels[k:k + 1, :], (LANES, LANES)).T
        spare = lax.broadcasted_iota(jnp.int32, (LANES, LANES), 1)
        rows = pl.ds(k * LANES, LANES)
        own_ref[rows, :] = jnp.where(spare == LAB, column, 0.0).astype(jnp.bfloat16)
        own_ref[rows, :num_feat] = x_in[rows, :]
    chain_row = lax.broadcasted_iota(jnp.int32, (hidden, 8, num_feat), 1) == chip % 8
    chain_lane = lax.broadcasted_iota(jnp.int32, wo_ref.shape, 1) == chip
    for n, ref in enumerate((pos_ref, vel_ref)):
        ref[:hidden, :num_feat] = jnp.sum(jnp.where(chain_row, w_tmp[n], 0.0), axis=1)
        ref[:hidden, OUT:OUT + 1] = jnp.sum(jnp.where(chain_lane, o_tmp[n], 0.0), axis=1, keepdims=True)


def collect_rows(own_ref, pos_ref, x_all, xt_all, y_all, part_ref, w2_ref, wbd_ref, a_ref, zp_ref, b_ref, g_ref, acc_ref,
                 x_send, x_recv, own_sem):
    core, chip, coords, partner, device_at = place()
    own = pltpu.make_async_copy(own_ref, x_all.at[coords[0], coords[1], coords[2]], own_sem)
    own.start()
    ready = greet(torus_neighbours(coords, device_at))
    g_ref[...] = jnp.zeros_like(g_ref)
    acc_ref[...] = jnp.zeros_like(acc_ref)
    set_weights(pos_ref[...], wbd_ref, w2_ref)
    own.wait()
    ready()

    def forward(b):
        wbd = jnp.concatenate([wbd_ref[0], wbd_ref[1]], axis=1)
        pres = []
        for t in range(2):
            tiles = [jnp.concatenate([xt_all[b, 4 * s + 2 * t], xt_all[b, 4 * s + 2 * t + 1]], axis=1) for s in range(2)]
            pres.append(jnp.dot(wbd, jnp.concatenate(tiles, axis=0), preferred_element_type=jnp.float32))
        return pres

    def activate(pres, u):
        w2 = w2_ref[...].reshape(HID // 8, 8, LANES)
        for t in range(2):
            act = jnp.tanh(pres[t])
            for h in range(2):
                j = 2 * t + h
                a_ref[u, j] = act[:, h * LANES:(h + 1) * LANES]
                for s in range(2):
                    part = act[s * HID:(s + 1) * HID, h * LANES:(h + 1) * LANES].reshape(HID // 8, 8, LANES)
                    k = 4 * s + j
                    zp_ref[u, 8 * k:8 * k + 8, :] = jnp.sum(part * w2, axis=0)

    def backward(b, u, acc):
        z = zp_ref[u, pl.ds(0, 8, stride=8), :]
        for k in range(1, 8):
            z = z + zp_ref[u, pl.ds(k, 8, stride=8), :]
        res = y_all[b] - 1.0 / (1.0 + jnp.exp(-z))
        w2 = w2_ref[...]
        for j in range(4):
            parts = []
            for s in range(2):
                r = jnp.broadcast_to(res[4 * s + j:4 * s + j + 1, :], (HID, LANES))
                act = a_ref[u, j, s * HID:(s + 1) * HID, :]
                ra = r * act
                acc = acc + ra
                parts.append((r - ra * act) * w2)
            b_ref[u, j] = jnp.concatenate(parts, axis=0).astype(jnp.bfloat16)
        return acc

    def weight_grad(where, u):
        z, y, x = where
        rows = x_all.at[z, y, x]
        lhs = jnp.concatenate([b_ref[u, j] for j in range(4)], axis=1)
        return jnp.dot(lhs, jnp.concatenate([rows[:512, :], rows[512:, :]], axis=1), preferred_element_type=jnp.float32)

    def digest(wheres):
        blocks = [(z * SIDE + y) * SIDE + x for z, y, x in wheres]
        for where in wheres:
            turn(where)
        for u, b in enumerate(blocks):
            activate(forward(b), u)
        acc = acc_ref[...]
        for u, b in enumerate(blocks):
            acc = backward(b, u, acc)
        acc_ref[...] = acc
        part = weight_grad(wheres[0], 0)
        for u in range(1, len(wheres)):
            part = part + weight_grad(wheres[u], u)
        g_ref[...] += part

    def turn(where):
        z, y, x = where
        b = (z * SIDE + y) * SIDE + x
        for k in range(8):
            xt = x_all[z, y, x, k * LANES:(k + 1) * LANES, :].T
            xt_all[b, k] = xt
            y_all[b, k:k + 1, :] = xt[112:128, :].astype(jnp.float32)[LAB - 112:LAB - 111, :]

    def moved(offsets):
        return tuple(lax.rem(c + o, SIDE) for c, o in zip(coords, offsets))

    def three(i):
        return 3 + i

    def near():
        def body(i, carry):
            digest([moved((three(i), three(j // 3), three(j % 3))) for j in range(9)])
            return carry
        lax.fori_loop(0, 3, body, 0)

    def middle():
        def body(i, carry):
            u = three(i)
            digest([moved(o) for v in (three(0), three(1), three(2)) for o in ((2, u, v), (u, 2, v), (u, v, 2))])
            return carry
        lax.fori_loop(0, 3, body, 0)

    def far():
        digest([moved(o) for v in (three(0), three(1), three(2)) for o in ((2, 2, v), (2, v, 2), (v, 2, 2))] + [moved((2, 2, 2))])

    x_descs = torus_gather(x_all, ROW_PIECES, coords, device_at, x_send, x_recv, near, middle)
    far()
    for d in x_descs:
        d.wait_send()
    part_ref[...] = whole_gradient(g_ref[...], acc_ref[...])


def gradient(with_loss, *refs):
    def with_acc(pre, grad):
        gradient_body(with_loss, pre, grad, *refs)

    def spec(q):
        return pltpu.ACC(q)((2 * HID, 2 * LANES), jnp.float32)

    pl.run_scoped(with_acc, ((spec(0), spec(1)), (spec(0), spec(1))), (spec(0), spec(1)))


def gradient_body(with_loss, pre_acc, grad_acc, x_all, xt_all, y_all, pos_ref, part_ref, z_all, w2_ref, wbd_ref, b_ref):
    lane, sub = grids()
    def push_forward(b, qs=(0, 1)):
        for q in qs:
            tiles = [jnp.concatenate([xt_all[b, 4 * s + 2 * q], xt_all[b, 4 * s + 2 * q + 1]], axis=1) for s in range(2)]
            pltpu.matmul_push_rhs(jnp.concatenate(tiles, axis=0), staging_register=0, mxu_index=q)

    def forward(u, qs=(0, 1)):
        wbd = jnp.concatenate([wbd_ref[0], wbd_ref[1]], axis=1)
        for q in qs:
            pltpu.matmul_acc_lhs(pre_acc[u][q], wbd, load_staged_rhs=0)

    def rows_to_back(b, u, acc, qs=(0, 1)):
        w2 = w2_ref[...].reshape(HID // 8, 8, LANES)
        for q in qs:
            act = jnp.tanh(pltpu.matmul_pop(pre_acc[u][q]))
            for h in range(2):
                j = 2 * q + h
                parts = []
                for s in range(2):
                    k = 4 * s + j
                    part = act[s * HID:(s + 1) * HID, h * LANES:(h + 1) * LANES].reshape(HID // 8, 8, LANES)
                    z = jnp.sum(part * w2, axis=0)
                    for shift in (4, 2, 1):
                        z = z + pltpu.roll(z, shift, 0)
                    if with_loss:
                        z_all[b, k:k + 1, :] = z[:1]
                    res = jnp.broadcast_to(y_all[b, k:k + 1, :], (8, LANES)) - 1.0 / (1.0 + jnp.exp(-z))
                    weighed = part * res
                    acc = acc + weighed
                    parts.append(((res - weighed * part) * w2).reshape(HID, LANES))
                b_ref[u, j] = jnp.concatenate(parts, axis=0).astype(jnp.bfloat16)
        return acc

    def push_grad(b, qs=(0, 1)):
        z, y, x = block_index(b)
        rows = x_all.at[z, y, x]
        for q in qs:
            tile = jnp.concatenate([rows[256 * q:256 * q + 256, :], rows[512 + 256 * q:768 + 256 * q, :]], axis=1)
            pltpu.matmul_push_rhs(tile, staging_register=1, mxu_index=q)

    def weight_grad(u, qs=(0, 1)):
        for q in qs:
            lhs = jnp.concatenate([b_ref[u, 2 * q], b_ref[u, 2 * q + 1]], axis=1)
            pltpu.matmul_acc_lhs(grad_acc[q], lhs, load_staged_rhs=1)

    pos = pos_ref[...]
    w_in = jnp.where(lane < LAB, pos, 0.0)
    nil = jnp.zeros_like(w_in)
    wbd_ref[0] = jnp.concatenate([w_in, nil], axis=0).astype(jnp.bfloat16)
    wbd_ref[1] = jnp.concatenate([nil, w_in], axis=0).astype(jnp.bfloat16)
    w2_ref[...] = jnp.broadcast_to(pos[:, OUT:OUT + 1], (HID, LANES))
    b_ref[1] = jnp.zeros((4, 2 * HID, LANES), jnp.bfloat16)
    for u in range(2):
        push_forward(u)
        forward(u)
    push_forward(2)
    push_grad(0)

    def pair(i, acc):
        for v in range(UNROLL):
            u = v % 2
            n = UNROLL * i + v
            acc = rows_to_back(n, u, acc, (0,))
            forward(u, (0,))
            push_forward(jnp.minimum(n + 3, BLOCKS - 1), (0,))
            weight_grad(1 - u, (0,))
            push_grad(n, (0,))
            acc = rows_to_back(n, u, acc, (1,))
            forward(u, (1,))
            push_forward(jnp.minimum(n + 3, BLOCKS - 1), (1,))
            weight_grad(1 - u, (1,))
            push_grad(n, (1,))
        return acc

    acc = lax.fori_loop(0, BLOCKS // UNROLL, pair, jnp.zeros((HID // 8, 8, LANES), jnp.float32)).reshape(HID, LANES)
    weight_grad(1)
    whole = pltpu.matmul_pop(grad_acc[0]) + pltpu.matmul_pop(grad_acc[1])
    forward(0)
    for u in range(2):
        for q in range(2):
            pltpu.matmul_pop(pre_acc[u][q])
    grad = whole[:HID, :LANES] + whole[HID:, LANES:]
    grad = jnp.where(lane < LAB, grad, jnp.where(lane == OUT, jnp.sum(acc, axis=1, keepdims=True), 0.0))
    if with_loss:
        def loss_block(b, total):
            z = z_all[b]
            return total + (jnp.maximum(z, 0.0) + jnp.log1p(jnp.exp(-jnp.abs(z))) - y_all[b] * z)

        total = lax.fori_loop(0, BLOCKS, loss_block, jnp.zeros((8, LANES), jnp.float32))
        total = jnp.sum(jnp.sum(total, axis=1, keepdims=True), axis=0, keepdims=True)
        grad = jnp.where((lane == LOSS) & (sub == 0), total, grad)
    part_ref[...] = grad


def both_parts(part_ref, rcv, partner, e_send, e_recv):
    ex = pltpu.make_async_remote_copy(
        src_ref=part_ref, dst_ref=rcv, send_sem=e_send, recv_sem=e_recv,
        device_id={'data': partner}, device_id_type=pl.DeviceIdType.MESH)
    ex.start()
    ex.wait()
    return part_ref[...] + rcv[...]


def kick(vel, pos, total, rate):
    lane, _ = grids()
    is_param = (lane < LAB) | (lane == OUT)
    return vel + rate * jnp.where(is_param, total - pos * (1.0 / PRIOR_VAR), 0.0)


def leap(rate, step_size, part_ref, pos_ref, vel_ref, pos_new, vel_new, rcv, e_send, e_recv):
    _, _, _, partner, _ = place()
    greet([partner])()
    total = both_parts(part_ref, rcv, partner, e_send, e_recv)
    vel = kick(vel_ref[...], pos_ref[...], total, rate)
    vel_new[...] = vel
    pos_new[...] = pos_ref[...] + step_size * vel


def finish(rate, hidden, part_ref, pos_ref, vel_ref, all_ref, rcv, e_send, e_recv, o_send, o_recv, s_send, s_recv):
    core, _, coords, partner, device_at = place()
    greet(torus_neighbours(coords, device_at, (1, -1, 2)) + [partner])()
    total = both_parts(part_ref, rcv, partner, e_send, e_recv)
    lane, sub = grids()
    pos = pos_ref[...]
    vel = kick(vel_ref[...], pos, total, rate)
    loss = total[:1, LOSS:LOSS + 1]
    square = (pos * pos) * (1.0 / (2.0 * PRIOR_VAR)) + 0.5 * (vel * vel)
    energy = loss + jnp.sum(jnp.sum(square, axis=1, keepdims=True), axis=0, keepdims=True)
    tails = []
    for value in (pos, vel):
        w2 = jnp.broadcast_to(value[:, OUT:OUT + 1], (HID, LANES))
        row = jnp.concatenate([w2, jnp.zeros((LANES - HID, LANES), jnp.float32)], axis=0).T[:1, :]
        tails.append(jnp.broadcast_to(row, (HID, LANES)))
    tails[0] = jnp.where(lane == hidden, energy, tails[0])
    outs = [jnp.where(sub == hidden, t, v) for t, v in zip(tails, (pos, vel))]
    all_ref[core, coords[0], coords[1], coords[2]] = jnp.where(core == 0, outs[0], outs[1])
    shared = []

    def across(side, p, i, where):
        start, size, _ = OUT_PIECES[p]
        ref = all_ref.at[side, where[0], where[1], where[2], pl.ds(start, size), :]
        return pltpu.make_async_remote_copy(
            src_ref=ref, dst_ref=ref, send_sem=s_send.at[p, i], recv_sem=s_recv.at[p, i],
            device_id={'data': partner}, device_id_type=pl.DeviceIdType.MESH)

    def share(p, i, where):
        across(core, p, i, where).start()
        shared.append((p, i, where))

    o_descs = torus_gather(all_ref.at[core], OUT_PIECES, coords, device_at, o_send, o_recv, share=share)
    for d in o_descs:
        d.wait_send()
    for item in shared:
        across(core, *item).wait_send()
        across(1 - core, *item).wait_recv()


def spread_out(flat, w_end, wo_end, m_end, mo_end, e_end):
    hidden, _, num_feat = w_end.shape

    def spread(h, carry):
        for n, ref in enumerate((w_end, m_end)):
            for c in range(0, BLOCKS, 8):
                ref[h, c:c + 8, :] = flat[n, pl.ds(c * HID + h, 8, stride=HID), :][:, :num_feat]
        return carry

    lax.fori_loop(0, hidden, spread, 0)
    for n, ref in enumerate((wo_end, mo_end)):
        tail = jnp.concatenate([flat[n, pl.ds(c * HID + hidden, 8, stride=HID), :] for c in range(0, BLOCKS, 8)]
                               + [jnp.zeros((LANES - BLOCKS, LANES), jnp.float32)], axis=0).T
        ref[...] = tail[:hidden, :BLOCKS]
        if n == 0:
            e_end[...] = tail[hidden:hidden + 1, :BLOCKS]


VMEM = pl.BlockSpec(memory_space=pltpu.VMEM)
HBM = pl.BlockSpec(memory_space=pltpu.HBM)
DMA = pltpu.SemaphoreType.DMA


def struct(shape, dtype=jnp.float32):
    return jax.ShapeDtypeStruct(shape, dtype)


def call(kernel, name, inputs, outs, scratch, limit, collective=None, in_specs=None):
    extra = {} if collective is None else dict(collective_id=collective, has_side_effects=True)
    return pl.pallas_call(
        kernel, out_shape=outs, in_specs=in_specs or [VMEM] * len(inputs),
        out_specs=[VMEM] * len(outs) if isinstance(outs, list) else VMEM, scratch_shapes=scratch,
        compiler_params=pltpu.CompilerParams(vmem_limit_bytes=limit, **extra), name=name)(*inputs)


def grad_call(data, pos, with_loss):
    bf16 = jnp.bfloat16
    return call(functools.partial(gradient, with_loss), 'gradient', (*data, pos), struct((HID, LANES)), [
        pltpu.VMEM((BLOCKS, 8, LANES), jnp.float32),
        pltpu.VMEM((HID, LANES), jnp.float32),
        pltpu.VMEM((2, 2 * HID, LANES), bf16),
        pltpu.VMEM((2, 4, 2 * HID, LANES), bf16)], 4 * MIB)


def run_all(feats, labels, w_in, w_out, mom_in, mom_out, step_size):
    rows, num_feat = feats.shape
    hidden, chains, _ = w_in.shape
    f32, bf16 = jnp.float32, jnp.bfloat16
    state = struct((HID, LANES))
    own, pos, vel = call(
        prepare, 'prepare', (feats, labels, w_in, w_out, mom_in, mom_out), [struct((rows, LANES), bf16), state, state],
        [pltpu.VMEM((rows, num_feat), bf16), pltpu.VMEM((2, hidden, 8, num_feat), f32), pltpu.VMEM((8, LANES), jnp.int32), pltpu.VMEM((2, hidden, chains), f32), DMA((6,))],
        PREPARE_BYTES, None, [HBM] * 6)
    outs = [struct((SIDE, SIDE, SIDE, rows, LANES), bf16), struct((BLOCKS, rows // LANES, LANES, LANES), bf16), struct((BLOCKS, 8, LANES))]
    *data, part = call(collect_rows, 'collect', (own, pos), outs + [state], [
        pltpu.VMEM((HID, LANES), f32), pltpu.VMEM((2, 2 * HID, LANES), bf16), pltpu.VMEM((10, 4, 2 * HID, LANES), f32),
        pltpu.VMEM((10, 64, LANES), f32), pltpu.VMEM((10, 4, 2 * HID, LANES), bf16), pltpu.VMEM((2 * HID, 2 * LANES), f32),
        pltpu.VMEM((HID, LANES), f32), DMA((3, 36)), DMA((3, 36)), DMA], 8 * MIB, 0)
    for k in range(LEAPS):
        if k > 0:
            part = grad_call(data, pos, False)
        rate = 0.5 * step_size if k == 0 else step_size
        pos, vel = call(functools.partial(leap, rate, step_size), 'leap', (part, pos, vel), [state, state],
                        [pltpu.VMEM((HID, LANES), f32), DMA, DMA], MIB, 1 if k == 0 else 2)
    part = grad_call(data, pos, True)
    every = call(functools.partial(finish, 0.5 * step_size, hidden), 'finish', (part, pos, vel), struct((2, SIDE, SIDE, SIDE, HID, LANES)),
                 [pltpu.VMEM((HID, LANES), f32), DMA, DMA, DMA((3, 36)), DMA((3, 36)), DMA((3, 4)), DMA((3, 4))], 2 * MIB, 3)
    ends = [struct(w_in.shape), struct(w_out.shape)] * 2 + [struct((1, chains))]
    return call(spread_out, 'spread', (every.reshape(2, BLOCKS * HID, LANES),), ends, [], 8 * MIB)


def solution(mesh):
    row_spec = P('data', None)
    label_spec = P('data')
    in_spec = P(None, 'parts', None)
    out_spec = P('parts', None)
    chain_spec = P('parts')

    def run_chains(feats, labels, w_in, w_out, mom_in, mom_out):
        num_rows, num_feat = feats.shape
        hidden = w_in.shape[2]
        step_size = 1.0 / math.sqrt(num_rows * (num_feat + hidden))

        def device_body(x_rows, y_rows, pos_in, pos_out, vel_in, vel_out):
            turned = [jnp.transpose(v) for v in (pos_in, pos_out, vel_in, vel_out)]
            ends = run_all(x_rows, y_rows.reshape(8, LANES), *turned, step_size)
            return tuple(jnp.transpose(v) for v in ends[:4]) + (ends[4].reshape(-1),)

        mapped = jax.shard_map(device_body, mesh=mesh, in_specs=(row_spec, label_spec, in_spec, out_spec, in_spec, out_spec), out_specs=(in_spec, out_spec, in_spec, out_spec, chain_spec), check_vma=False)
        return mapped(feats, labels, w_in, w_out, mom_in, mom_out)

    return run_chains
```

```python
import functools
import math

import jax
import jax.numpy as jnp
from jax import lax
from jax.experimental import pallas as pl
from jax.experimental.pallas import tpu as pltpu
from jax.sharding import PartitionSpec as P

LEAPS = 16
PRIOR_VAR = 1.0
SIDE = 4
BLOCKS = SIDE ** 3
HID = 56
LANES = 128
LAB = 123
LOSS = 124
OUT = 127
UNROLL = 8
MIB = 2 ** 20
PREPARE_BYTES = 57000000
ROW_PIECES = ((0, 344, 176), (344, 344, 176), (688, 336, 168))
OUT_PIECES = ((0, 24, 16), (24, 16, 8), (40, 16, 8))


def torus_gather(buf, pieces, coords, device_at, send_sem, recv_sem, near=None, middle=None, share=None):
    descs = []
    direct = share is not None
    plus = lambda c, d: lax.rem(c + d + SIDE, SIDE)

    def view(p, where, part):
        start, size, first = pieces[p]
        lo, n = {0: (start, size), 1: (start, first), 2: (start + first, size - first)}[part]
        return buf.at[where[0], where[1], where[2], pl.ds(lo, n), :]

    def copy(p, where, part, axis, step, slot):
        to = list(coords)
        to[axis] = plus(to[axis], step)
        ref = view(p, where, part)
        return pltpu.make_async_remote_copy(
            src_ref=ref, dst_ref=ref, send_sem=send_sem.at[p, slot], recv_sem=recv_sem.at[p, slot],
            device_id={'data': device_at(to)}, device_id_type=pl.DeviceIdType.MESH)

    def send(p, where, part, axis, step, slot):
        c = copy(p, where, part, axis, step, slot)
        c.start()
        descs.append(c)

    def wait(p, where, part, axis, step, slot):
        copy(p, where, part, axis, step, slot).wait_recv()

    orders = [(p, (p + 1) % 3, (p + 2) % 3) for p in range(3)]
    OFFS = (0, -1, 1, 2)

    def at(p, off0, off1, off2):
        where = [None, None, None]
        for axis, off in zip(orders[p], (off0, off1, off2)):
            where[axis] = slice(None) if off is None else (coords[axis] if off == 0 else plus(coords[axis], off))
        return where

    def start_full(p, ph, own, base):
        axis = orders[p][ph]
        send(p, own, 0, axis, 1, base)
        send(p, own, 0, axis, -1, base + 1)
        if direct and ph < 2:
            send(p, own, 0, axis, 2, base + 2)

    def relay(p, ph, low, high, base):
        axis = orders[p][ph]
        wait(p, low, 0, axis, 1, base)
        if direct and ph < 2:
            wait(p, high, 0, axis, 1, base + 1)
            return
        send(p, low, 1, axis, 1, base + 2)
        wait(p, high, 0, axis, 1, base + 1)
        send(p, high, 2, axis, -1, base + 3)

    def finish(p, ph, far, base):
        axis = orders[p][ph]
        if direct and ph < 2:
            wait(p, far, 0, axis, 1, base + 2)
            return
        wait(p, far, 1, axis, 1, base + 2)
        wait(p, far, 2, axis, 1, base + 3)

    B1, B2, B3 = 0, 4, 20
    for p in range(3):
        start_full(p, 0, at(p, 0, 0, 0), B1)
    for p in range(3):
        start_full(p, 1, at(p, 0, 0, 0), B2)
    for p in range(3):
        relay(p, 0, at(p, -1, 0, 0), at(p, 1, 0, 0), B1)
        start_full(p, 1, at(p, -1, 0, 0), B2 + 4)
        start_full(p, 1, at(p, 1, 0, 0), B2 + 8)
    for p in range(3):
        finish(p, 0, at(p, 2, 0, 0), B1)
        start_full(p, 1, at(p, 2, 0, 0), B2 + 12)
        start_full(p, 2, at(p, None, 0, 0), B3)
    for q in range(4):
        for p in range(3):
            relay(p, 1, at(p, OFFS[q], -1, 0), at(p, OFFS[q], 1, 0), B2 + 4 * q)
    for p in range(3):
        start_full(p, 2, at(p, None, -1, 0), B3 + 4)
        start_full(p, 2, at(p, None, 1, 0), B3 + 8)
    for q in range(4):
        for p in range(3):
            finish(p, 1, at(p, OFFS[q], 2, 0), B2 + 4 * q)
    for p in range(3):
        start_full(p, 2, at(p, None, 2, 0), B3 + 12)
    for q in range(4):
        if q == 3 and near is not None:
            near()
        for p in range(3):
            relay(p, 2, at(p, None, OFFS[q], -1), at(p, None, OFFS[q], 1), B3 + 4 * q)
    if share is not None:
        for p in range(3):
            for i in range(3):
                share(p, i, at(p, None, None, OFFS[i]))
    for q in range(4):
        for p in range(3):
            finish(p, 2, at(p, None, OFFS[q], 2), B3 + 4 * q)
        if q < 3 and middle is not None:
            middle(q)
    if share is not None:
        for p in range(3):
            share(p, 3, at(p, None, None, 2))
    return descs


def block_index(b):
    return b // (SIDE * SIDE), (b // SIDE) % SIDE, b % SIDE


def place():
    me = lax.axis_index('data')
    core = me % 2
    chip = me // 2
    coords = (chip // (SIDE * SIDE), (chip // SIDE) % SIDE, chip % SIDE)

    def device_at(c):
        return ((c[0] * SIDE + c[1]) * SIDE + c[2]) * 2 + core

    return core, chip, coords, me + 1 - 2 * core, device_at


def greet(devices):
    barrier = pltpu.get_barrier_semaphore()
    for device in devices:
        pl.semaphore_signal(barrier, inc=1, device_id={'data': device}, device_id_type=pl.DeviceIdType.MESH)
    return lambda: pl.semaphore_wait(barrier, len(devices))


def torus_neighbours(coords, device_at, steps=(1, -1)):
    found = []
    for axis in range(3):
        for step in steps:
            to = list(coords)
            to[axis] = lax.rem(to[axis] + step + SIDE, SIDE)
            found.append(device_at(to))
    return found


def grids():
    lane = lax.broadcasted_iota(jnp.int32, (HID, LANES), 1)
    sub = lax.broadcasted_iota(jnp.int32, (HID, LANES), 0)
    return lane, sub


def set_weights(pos, wbd_ref, w2_ref):
    lane, _ = grids()
    w_in = jnp.where(lane < LAB, pos, 0.0)
    nil = jnp.zeros_like(w_in)
    wbd_ref[0] = jnp.concatenate([w_in, nil], axis=0).astype(jnp.bfloat16)
    wbd_ref[1] = jnp.concatenate([nil, w_in], axis=0).astype(jnp.bfloat16)
    w2_ref[...] = jnp.broadcast_to(pos[:, OUT:OUT + 1], (HID, LANES))


def whole_gradient(whole, acc):
    lane, _ = grids()
    grad = whole[:HID, :LANES] + whole[HID:, LANES:]
    return jnp.where(lane < LAB, grad, jnp.where(lane == OUT, jnp.sum(acc, axis=1, keepdims=True), 0.0))


def prepare(feat_ref, lab_ref, w_ref, wo_ref, m_ref, mo_ref, own_ref, pos_ref, vel_ref, x_in, w_tmp, lab_tmp, o_tmp, sem):
    num_feat = feat_ref.shape[1]
    hidden = w_ref.shape[0]
    chip = lax.axis_index('data') // 2
    eight = pl.multiple_of((chip // 8) * 8, 8)
    loads = [pltpu.make_async_copy(feat_ref, x_in, sem.at[0]), pltpu.make_async_copy(lab_ref, lab_tmp, sem.at[1])]
    for n, ref in enumerate((w_ref, m_ref)):
        loads.append(pltpu.make_async_copy(ref.at[:, pl.ds(eight, 8), :], w_tmp.at[n], sem.at[n + 2]))
    for n, ref in enumerate((wo_ref, mo_ref)):
        loads.append(pltpu.make_async_copy(ref, o_tmp.at[n], sem.at[n + 4]))
    for load in loads:
        load.start()
    pos_ref[...] = jnp.zeros_like(pos_ref)
    vel_ref[...] = jnp.zeros_like(vel_ref)
    for load in loads:
        load.wait()
    labels = lab_tmp[...].astype(jnp.float32)
    for k in range(8):
        column = jnp.broadcast_to(labels[k:k + 1, :], (LANES, LANES)).T
        spare = lax.broadcasted_iota(jnp.int32, (LANES, LANES), 1)
        rows = pl.ds(k * LANES, LANES)
        own_ref[rows, :] = jnp.where(spare == LAB, column, 0.0).astype(jnp.bfloat16)
        own_ref[rows, :num_feat] = x_in[rows, :]
    chain_row = lax.broadcasted_iota(jnp.int32, (hidden, 8, num_feat), 1) == chip % 8
    chain_lane = lax.broadcasted_iota(jnp.int32, wo_ref.shape, 1) == chip
    for n, ref in enumerate((pos_ref, vel_ref)):
        ref[:hidden, :num_feat] = jnp.sum(jnp.where(chain_row, w_tmp[n], 0.0), axis=1)
        ref[:hidden, OUT:OUT + 1] = jnp.sum(jnp.where(chain_lane, o_tmp[n], 0.0), axis=1, keepdims=True)


def collect_rows(own_ref, pos_ref, x_all, xt_all, y_all, part_ref, w2_ref, wbd_ref, a_ref, zp_ref, b_ref, g_ref, acc_ref,
                 x_send, x_recv, own_sem):
    core, chip, coords, partner, device_at = place()
    own = pltpu.make_async_copy(own_ref, x_all.at[coords[0], coords[1], coords[2]], own_sem)
    own.start()
    ready = greet(torus_neighbours(coords, device_at))
    g_ref[...] = jnp.zeros_like(g_ref)
    acc_ref[...] = jnp.zeros_like(acc_ref)
    set_weights(pos_ref[...], wbd_ref, w2_ref)
    own.wait()
    ready()

    def forward(b):
        wbd = jnp.concatenate([wbd_ref[0], wbd_ref[1]], axis=1)
        pres = []
        for t in range(2):
            tiles = [jnp.concatenate([xt_all[b, 4 * s + 2 * t], xt_all[b, 4 * s + 2 * t + 1]], axis=1) for s in range(2)]
            pres.append(jnp.dot(wbd, jnp.concatenate(tiles, axis=0), preferred_element_type=jnp.float32))
        return pres

    def activate(pres, u):
        w2 = w2_ref[...].reshape(HID // 8, 8, LANES)
        for t in range(2):
            act = jnp.tanh(pres[t])
            for h in range(2):
                j = 2 * t + h
                a_ref[u, j] = act[:, h * LANES:(h + 1) * LANES]
                for s in range(2):
                    part = act[s * HID:(s + 1) * HID, h * LANES:(h + 1) * LANES].reshape(HID // 8, 8, LANES)
                    k = 4 * s + j
                    zp_ref[u, 8 * k:8 * k + 8, :] = jnp.sum(part * w2, axis=0)

    def backward(b, u, acc):
        z = zp_ref[u, pl.ds(0, 8, stride=8), :]
        for k in range(1, 8):
            z = z + zp_ref[u, pl.ds(k, 8, stride=8), :]
        res = y_all[b] - 1.0 / (1.0 + jnp.exp(-z))
        w2 = w2_ref[...]
        for j in range(4):
            parts = []
            for s in range(2):
                r = jnp.broadcast_to(res[4 * s + j:4 * s + j + 1, :], (HID, LANES))
                act = a_ref[u, j, s * HID:(s + 1) * HID, :]
                ra = r * act
                acc = acc + ra
                parts.append((r - ra * act) * w2)
            b_ref[u, j] = jnp.concatenate(parts, axis=0).astype(jnp.bfloat16)
        return acc

    def weight_grad(where, u):
        z, y, x = where
        rows = x_all.at[z, y, x]
        lhs = jnp.concatenate([b_ref[u, j] for j in range(4)], axis=1)
        return jnp.dot(lhs, jnp.concatenate([rows[:512, :], rows[512:, :]], axis=1), preferred_element_type=jnp.float32)

    def digest(wheres):
        blocks = [(z * SIDE + y) * SIDE + x for z, y, x in wheres]
        for where in wheres:
            turn(where)
        for u, b in enumerate(blocks):
            activate(forward(b), u)
        acc = acc_ref[...]
        for u, b in enumerate(blocks):
            acc = backward(b, u, acc)
        acc_ref[...] = acc
        part = weight_grad(wheres[0], 0)
        for u in range(1, len(wheres)):
            part = part + weight_grad(wheres[u], u)
        g_ref[...] += part

    def turn(where):
        z, y, x = where
        b = (z * SIDE + y) * SIDE + x
        for k in range(8):
            xt = x_all[z, y, x, k * LANES:(k + 1) * LANES, :].T
            xt_all[b, k] = xt
            y_all[b, k:k + 1, :] = xt[112:128, :].astype(jnp.float32)[LAB - 112:LAB - 111, :]

    def moved(offsets):
        return tuple(lax.rem(c + o, SIDE) for c, o in zip(coords, offsets))

    def three(i):
        return 3 + i

    def near():
        def body(i, carry):
            digest([moved((three(i), three(j // 3), three(j % 3))) for j in range(9)])
            return carry
        lax.fori_loop(0, 3, body, 0)

    def middle(q):
        u = (0, 3, 1)[q]
        digest([moved(o) for v in (0, 3, 1) for o in ((v, u, 2), (2, v, u), (u, 2, v))])

    def far():
        digest([moved(o) for v in (three(0), three(1), three(2)) for o in ((2, 2, v), (2, v, 2), (v, 2, 2))] + [moved((2, 2, 2))])

    x_descs = torus_gather(x_all, ROW_PIECES, coords, device_at, x_send, x_recv, near, middle)
    far()
    for d in x_descs:
        d.wait_send()
    part_ref[...] = whole_gradient(g_ref[...], acc_ref[...])


def gradient(with_loss, *refs):
    def with_acc(pre, grad):
        gradient_body(with_loss, pre, grad, *refs)

    def spec(q):
        return pltpu.ACC(q)((2 * HID, 2 * LANES), jnp.float32)

    pl.run_scoped(with_acc, ((spec(0), spec(1)), (spec(0), spec(1))), (spec(0), spec(1)))


def gradient_body(with_loss, pre_acc, grad_acc, x_all, xt_all, y_all, pos_ref, part_ref, z_all, w2_ref, wbd_ref, b_ref):
    lane, sub = grids()
    def push_forward(b, qs=(0, 1)):
        for q in qs:
            tiles = [jnp.concatenate([xt_all[b, 4 * s + 2 * q], xt_all[b, 4 * s + 2 * q + 1]], axis=1) for s in range(2)]
            pltpu.matmul_push_rhs(jnp.concatenate(tiles, axis=0), staging_register=0, mxu_index=q)

    def forward(u, qs=(0, 1)):
        wbd = jnp.concatenate([wbd_ref[0], wbd_ref[1]], axis=1)
        for q in qs:
            pltpu.matmul_acc_lhs(pre_acc[u][q], wbd, load_staged_rhs=0)

    def rows_to_back(b, u, acc, qs=(0, 1)):
        w2 = w2_ref[...].reshape(HID // 8, 8, LANES)
        for q in qs:
            act = jnp.tanh(pltpu.matmul_pop(pre_acc[u][q]))
            for h in range(2):
                j = 2 * q + h
                parts = []
                for s in range(2):
                    k = 4 * s + j
                    part = act[s * HID:(s + 1) * HID, h * LANES:(h + 1) * LANES].reshape(HID // 8, 8, LANES)
                    z = jnp.sum(part * w2, axis=0)
                    for shift in (4, 2, 1):
                        z = z + pltpu.roll(z, shift, 0)
                    if with_loss:
                        z_all[b, k:k + 1, :] = z[:1]
                    res = jnp.broadcast_to(y_all[b, k:k + 1, :], (8, LANES)) - 1.0 / (1.0 + jnp.exp(-z))
                    weighed = part * res
                    acc = acc + weighed
                    parts.append(((res - weighed * part) * w2).reshape(HID, LANES))
                b_ref[u, j] = jnp.concatenate(parts, axis=0).astype(jnp.bfloat16)
        return acc

    def push_grad(b, qs=(0, 1)):
        z, y, x = block_index(b)
        rows = x_all.at[z, y, x]
        for q in qs:
            tile = jnp.concatenate([rows[256 * q:256 * q + 256, :], rows[512 + 256 * q:768 + 256 * q, :]], axis=1)
            pltpu.matmul_push_rhs(tile, staging_register=1, mxu_index=q)

    def weight_grad(u, qs=(0, 1)):
        for q in qs:
            lhs = jnp.concatenate([b_ref[u, 2 * q], b_ref[u, 2 * q + 1]], axis=1)
            pltpu.matmul_acc_lhs(grad_acc[q], lhs, load_staged_rhs=1)

    pos = pos_ref[...]
    w_in = jnp.where(lane < LAB, pos, 0.0)
    nil = jnp.zeros_like(w_in)
    wbd_ref[0] = jnp.concatenate([w_in, nil], axis=0).astype(jnp.bfloat16)
    wbd_ref[1] = jnp.concatenate([nil, w_in], axis=0).astype(jnp.bfloat16)
    w2_ref[...] = jnp.broadcast_to(pos[:, OUT:OUT + 1], (HID, LANES))
    b_ref[1] = jnp.zeros((4, 2 * HID, LANES), jnp.bfloat16)
    for u in range(2):
        push_forward(u)
        forward(u)
    push_forward(2)
    push_grad(0)

    def pair(i, acc):
        for v in range(UNROLL):
            u = v % 2
            n = UNROLL * i + v
            acc = rows_to_back(n, u, acc, (0,))
            forward(u, (0,))
            push_forward(jnp.minimum(n + 3, BLOCKS - 1), (0,))
            weight_grad(1 - u, (0,))
            push_grad(n, (0,))
            acc = rows_to_back(n, u, acc, (1,))
            forward(u, (1,))
            push_forward(jnp.minimum(n + 3, BLOCKS - 1), (1,))
            weight_grad(1 - u, (1,))
            push_grad(n, (1,))
        return acc

    acc = lax.fori_loop(0, BLOCKS // UNROLL, pair, jnp.zeros((HID // 8, 8, LANES), jnp.float32)).reshape(HID, LANES)
    weight_grad(1)
    whole = pltpu.matmul_pop(grad_acc[0]) + pltpu.matmul_pop(grad_acc[1])
    forward(0)
    for u in range(2):
        for q in range(2):
            pltpu.matmul_pop(pre_acc[u][q])
    grad = whole[:HID, :LANES] + whole[HID:, LANES:]
    grad = jnp.where(lane < LAB, grad, jnp.where(lane == OUT, jnp.sum(acc, axis=1, keepdims=True), 0.0))
    if with_loss:
        def loss_block(b, total):
            z = z_all[b]
            return total + (jnp.maximum(z, 0.0) + jnp.log1p(jnp.exp(-jnp.abs(z))) - y_all[b] * z)

        total = lax.fori_loop(0, BLOCKS, loss_block, jnp.zeros((8, LANES), jnp.float32))
        total = jnp.sum(jnp.sum(total, axis=1, keepdims=True), axis=0, keepdims=True)
        grad = jnp.where((lane == LOSS) & (sub == 0), total, grad)
    part_ref[...] = grad


def both_parts(part_ref, rcv, partner, e_send, e_recv):
    ex = pltpu.make_async_remote_copy(
        src_ref=part_ref, dst_ref=rcv, send_sem=e_send, recv_sem=e_recv,
        device_id={'data': partner}, device_id_type=pl.DeviceIdType.MESH)
    ex.start()
    ex.wait()
    return part_ref[...] + rcv[...]


def kick(vel, pos, total, rate):
    lane, _ = grids()
    is_param = (lane < LAB) | (lane == OUT)
    return vel + rate * jnp.where(is_param, total - pos * (1.0 / PRIOR_VAR), 0.0)


def leap(rate, step_size, part_ref, pos_ref, vel_ref, pos_new, vel_new, rcv, e_send, e_recv):
    _, _, _, partner, _ = place()
    greet([partner])()
    total = both_parts(part_ref, rcv, partner, e_send, e_recv)
    vel = kick(vel_ref[...], pos_ref[...], total, rate)
    vel_new[...] = vel
    pos_new[...] = pos_ref[...] + step_size * vel


def finish(rate, hidden, part_ref, pos_ref, vel_ref, all_ref, rcv, e_send, e_recv, o_send, o_recv, s_send, s_recv):
    core, _, coords, partner, device_at = place()
    greet(torus_neighbours(coords, device_at, (1, -1, 2)) + [partner])()
    total = both_parts(part_ref, rcv, partner, e_send, e_recv)
    lane, sub = grids()
    pos = pos_ref[...]
    vel = kick(vel_ref[...], pos, total, rate)
    loss = total[:1, LOSS:LOSS + 1]
    square = (pos * pos) * (1.0 / (2.0 * PRIOR_VAR)) + 0.5 * (vel * vel)
    energy = loss + jnp.sum(jnp.sum(square, axis=1, keepdims=True), axis=0, keepdims=True)
    tails = []
    for value in (pos, vel):
        w2 = jnp.broadcast_to(value[:, OUT:OUT + 1], (HID, LANES))
        row = jnp.concatenate([w2, jnp.zeros((LANES - HID, LANES), jnp.float32)], axis=0).T[:1, :]
        tails.append(jnp.broadcast_to(row, (HID, LANES)))
    tails[0] = jnp.where(lane == hidden, energy, tails[0])
    outs = [jnp.where(sub == hidden, t, v) for t, v in zip(tails, (pos, vel))]
    all_ref[core, coords[0], coords[1], coords[2]] = jnp.where(core == 0, outs[0], outs[1])
    shared = []

    def across(side, p, i, where):
        start, size, _ = OUT_PIECES[p]
        ref = all_ref.at[side, where[0], where[1], where[2], pl.ds(start, size), :]
        return pltpu.make_async_remote_copy(
            src_ref=ref, dst_ref=ref, send_sem=s_send.at[p, i], recv_sem=s_recv.at[p, i],
            device_id={'data': partner}, device_id_type=pl.DeviceIdType.MESH)

    def share(p, i, where):
        across(core, p, i, where).start()
        shared.append((p, i, where))

    o_descs = torus_gather(all_ref.at[core], OUT_PIECES, coords, device_at, o_send, o_recv, share=share)
    for d in o_descs:
        d.wait_send()
    for item in shared:
        across(core, *item).wait_send()
        across(1 - core, *item).wait_recv()


def spread_out(flat, w_end, wo_end, m_end, mo_end, e_end):
    hidden, _, num_feat = w_end.shape

    def spread(h, carry):
        for n, ref in enumerate((w_end, m_end)):
            for c in range(0, BLOCKS, 8):
                ref[h, c:c + 8, :] = flat[n, pl.ds(c * HID + h, 8, stride=HID), :][:, :num_feat]
        return carry

    lax.fori_loop(0, hidden, spread, 0)
    for n, ref in enumerate((wo_end, mo_end)):
        tail = jnp.concatenate([flat[n, pl.ds(c * HID + hidden, 8, stride=HID), :] for c in range(0, BLOCKS, 8)]
                               + [jnp.zeros((LANES - BLOCKS, LANES), jnp.float32)], axis=0).T
        ref[...] = tail[:hidden, :BLOCKS]
        if n == 0:
            e_end[...] = tail[hidden:hidden + 1, :BLOCKS]


VMEM = pl.BlockSpec(memory_space=pltpu.VMEM)
HBM = pl.BlockSpec(memory_space=pltpu.HBM)
DMA = pltpu.SemaphoreType.DMA


def struct(shape, dtype=jnp.float32):
    return jax.ShapeDtypeStruct(shape, dtype)


def call(kernel, name, inputs, outs, scratch, limit, collective=None, in_specs=None):
    extra = {} if collective is None else dict(collective_id=collective, has_side_effects=True)
    return pl.pallas_call(
        kernel, out_shape=outs, in_specs=in_specs or [VMEM] * len(inputs),
        out_specs=[VMEM] * len(outs) if isinstance(outs, list) else VMEM, scratch_shapes=scratch,
        compiler_params=pltpu.CompilerParams(vmem_limit_bytes=limit, **extra), name=name)(*inputs)


def grad_call(data, pos, with_loss):
    bf16 = jnp.bfloat16
    return call(functools.partial(gradient, with_loss), 'gradient', (*data, pos), struct((HID, LANES)), [
        pltpu.VMEM((BLOCKS, 8, LANES), jnp.float32),
        pltpu.VMEM((HID, LANES), jnp.float32),
        pltpu.VMEM((2, 2 * HID, LANES), bf16),
        pltpu.VMEM((2, 4, 2 * HID, LANES), bf16)], 4 * MIB)


def run_all(feats, labels, w_in, w_out, mom_in, mom_out, step_size):
    rows, num_feat = feats.shape
    hidden, chains, _ = w_in.shape
    f32, bf16 = jnp.float32, jnp.bfloat16
    state = struct((HID, LANES))
    own, pos, vel = call(
        prepare, 'prepare', (feats, labels, w_in, w_out, mom_in, mom_out), [struct((rows, LANES), bf16), state, state],
        [pltpu.VMEM((rows, num_feat), bf16), pltpu.VMEM((2, hidden, 8, num_feat), f32), pltpu.VMEM((8, LANES), jnp.int32), pltpu.VMEM((2, hidden, chains), f32), DMA((6,))],
        PREPARE_BYTES, None, [HBM] * 6)
    outs = [struct((SIDE, SIDE, SIDE, rows, LANES), bf16), struct((BLOCKS, rows // LANES, LANES, LANES), bf16), struct((BLOCKS, 8, LANES))]
    *data, part = call(collect_rows, 'collect', (own, pos), outs + [state], [
        pltpu.VMEM((HID, LANES), f32), pltpu.VMEM((2, 2 * HID, LANES), bf16), pltpu.VMEM((10, 4, 2 * HID, LANES), f32),
        pltpu.VMEM((10, 64, LANES), f32), pltpu.VMEM((10, 4, 2 * HID, LANES), bf16), pltpu.VMEM((2 * HID, 2 * LANES), f32),
        pltpu.VMEM((HID, LANES), f32), DMA((3, 36)), DMA((3, 36)), DMA], 8 * MIB, 0)
    for k in range(LEAPS):
        if k > 0:
            part = grad_call(data, pos, False)
        rate = 0.5 * step_size if k == 0 else step_size
        pos, vel = call(functools.partial(leap, rate, step_size), 'leap', (part, pos, vel), [state, state],
                        [pltpu.VMEM((HID, LANES), f32), DMA, DMA], MIB, 1 if k == 0 else 2)
    part = grad_call(data, pos, True)
    every = call(functools.partial(finish, 0.5 * step_size, hidden), 'finish', (part, pos, vel), struct((2, SIDE, SIDE, SIDE, HID, LANES)),
                 [pltpu.VMEM((HID, LANES), f32), DMA, DMA, DMA((3, 36)), DMA((3, 36)), DMA((3, 4)), DMA((3, 4))], 2 * MIB, 3)
    ends = [struct(w_in.shape), struct(w_out.shape)] * 2 + [struct((1, chains))]
    return call(spread_out, 'spread', (every.reshape(2, BLOCKS * HID, LANES),), ends, [], 8 * MIB)


def solution(mesh):
    row_spec = P('data', None)
    label_spec = P('data')
    in_spec = P(None, 'parts', None)
    out_spec = P('parts', None)
    chain_spec = P('parts')

    def run_chains(feats, labels, w_in, w_out, mom_in, mom_out):
        num_rows, num_feat = feats.shape
        hidden = w_in.shape[2]
        step_size = 1.0 / math.sqrt(num_rows * (num_feat + hidden))

        def device_body(x_rows, y_rows, pos_in, pos_out, vel_in, vel_out):
            turned = [jnp.transpose(v) for v in (pos_in, pos_out, vel_in, vel_out)]
            ends = run_all(x_rows, y_rows.reshape(8, LANES), *turned, step_size)
            return tuple(jnp.transpose(v) for v in ends[:4]) + (ends[4].reshape(-1),)

        mapped = jax.shard_map(device_body, mesh=mesh, in_specs=(row_spec, label_spec, in_spec, out_spec, in_spec, out_spec), out_specs=(in_spec, out_spec, in_spec, out_spec, chain_spec), check_vma=False)
        return mapped(feats, labels, w_in, w_out, mom_in, mom_out)

    return run_chains
```
